256 devices in a mesh: row: 16 (over z_hi, y), col: 16 (over z_lo, x, core).
Axes of the slice: x: 4, y: 4, z: 8 (z_hi: 4, z_lo: 2; z = z_hi * 2 + z_lo), core: 2. Of those that a mesh axis runs over, the one named last changes fastest.
Arguments:
- tokens: bfloat16 [8192, 4096], P('row', 'col'), may hold values from -6 to 6
- norm_gain: bfloat16 [4096], P('col'), may hold values from 0.099609375 to 1.8984375
- gate_weight: bfloat16 [4096, 10240], P('row', 'col'), may hold values from -0.09375 to 0.09375
- linear_weight: bfloat16 [4096, 10240], P('row', 'col'), may hold values from -0.09375 to 0.09375
- output_weight: bfloat16 [10240, 4096], P('col', 'row'), may hold values from -0.078125 to 0.078125
Outputs:
- block_out: bfloat16 [8192, 4096], P('row', 'col')
The draws below stay inside these ranges and needn't reach their ends.
All inputs are finite; a program needn't handle non-finite values.
Results may differ from the reference program's by a relative error of at most 0.0065.
Values may be sent and summed in bfloat16 or wider, within the bound.
A program may use at most 128 MiB of HBM per device.

```python
import jax
import jax.numpy as jnp
from jax import lax

D = 4096
FF = 10240
TOKENS = 8192


def raised(entries, key, source, target, shards_of, factor):
    owner, partner = [(jnp.arange(entries.shape[dim]) // (entries.shape[dim] // shards_of)).reshape([-1 if axis == dim else 1 for axis in range(entries.ndim)]) for dim in (source, target)]
    chosen = jax.random.permutation(key, shards_of)[partner]
    strong = (owner == chosen) | (owner == (partner + shards_of // 2) % shards_of)
    return jnp.where(strong, factor * entries, entries)


def steps_of(key, dims, pieces, low, high):
    def one(axis_at, shards_of):
        heights = jax.random.uniform(jax.random.fold_in(jax.random.fold_in(key, 6), axis_at), (shards_of,), jnp.float32, low / len(pieces), high / len(pieces))
        return jnp.repeat(jnp.exp(heights), dims[axis_at] // shards_of).reshape((-1,) + (1,) * (len(dims) - axis_at - 1))

    gain = one(*pieces[0])
    for cut in pieces[1:]:
        gain = gain * one(*cut)
    return gain


def scatter_about(key, shape, deviation, reach, pieces=(), dtype=jnp.bfloat16):
    array = deviation * jax.random.normal(key, shape, jnp.float32)
    if pieces:
        array = array * steps_of(key, shape, pieces, -0.22, 0.18)
    return jnp.clip(array, -reach, reach).astype(dtype)


def noise_with(rng, dims, width, bound, pieces, heavy, kind=jnp.bfloat16):
    result = width * jax.random.normal(rng, dims, jnp.float32)
    if pieces:
        result = result * steps_of(rng, dims, pieces, -0.22, 0.18)
    return jnp.clip(raised(result, jax.random.fold_in(rng, 3), *heavy), -bound, bound).astype(kind)


def setup_inputs(seed: int = 0) -> dict:
    key_of = jax.random.split(jax.random.key(seed), 6)
    return {
        "tokens": scatter_about(key_of[0], (TOKENS, D), 1.0, 6.0, ((0, 16), (1, 16))),
        "norm_gain": jnp.clip(1.0 + 0.18 * jax.random.normal(key_of[1], (D,), jnp.float32), 0.099609375, 1.8984375).astype(jnp.bfloat16),
        "gate_weight": scatter_about(key_of[2], (D, FF), D ** -0.5, 0.09375, ((0, 16), (1, 16))),
        "linear_weight": scatter_about(key_of[3], (D, FF), D ** -0.5, 0.09375, ((0, 16), (1, 16))),
        "output_weight": noise_with(key_of[4], (FF, D), FF ** -0.5, 0.078125, ((0, 16), (1, 16)), (0, 1, 16, 2.0)),
    }


def reference(tokens, norm_gain, gate_weight, linear_weight, output_weight):
    values = tokens.astype(jnp.float32)
    meansq = lax.optimization_barrier(jnp.mean(values * values, axis=-1, keepdims=True))
    normed = (values * jax.lax.rsqrt(meansq + 1e-06) * norm_gain.astype(jnp.float32)).astype(jnp.bfloat16)
    gate = jnp.dot(normed, gate_weight, preferred_element_type=jnp.float32)
    linear = jnp.dot(normed, linear_weight, preferred_element_type=jnp.float32)
    hidden = (jax.nn.gelu(gate, approximate=True) * linear).astype(jnp.bfloat16)
    return jnp.dot(hidden, output_weight, preferred_element_type=jnp.float32).astype(jnp.bfloat16)
```

```python
import jax
import jax.numpy as jnp
from jax import lax
from jax.experimental import pallas as pl
from jax.experimental.pallas import tpu as pltpu
from jax.sharding import PartitionSpec as P

MESH = pl.DeviceIdType.MESH
BF, F32 = jnp.bfloat16, jnp.float32
FB = 160
DB = 256
TB = 128
GR = 16
N_SEMS = 192
NT = (((1,), (1,)), ((), ()))


def wrap(v, n):
    return lax.rem(v + n, n)


def kernel(
    tok, gain, gw, lw, ow, out,
    wt, gl, w2, tst, tks, nrm, acc, hid, part, stx, srx, rtx, rrx, fin, land, send, recv,
):
    row, col = lax.axis_index("row"), lax.axis_index("col")
    zh, y = lax.div(row, 4), lax.rem(row, 4)
    zl, x, k = lax.div(col, 8), lax.rem(lax.div(col, 2), 4), lax.rem(col, 2)
    z = zh * 2 + zl

    def device(dz=0, dy=0, dx=0, dk=0):
        nz, ny, nx = wrap(z + dz, 8), wrap(y + dy, 4), wrap(x + dx, 4)
        return (lax.div(nz, 2) * 4 + ny, lax.rem(nz, 2) * 8 + nx * 2 + lax.rem(k + dk, 2))

    peers = (
        [device(dz=d) for d in (1, -1, 2, -2, 4)]
        + [device(dx=d) for d in (1, -1, 2)]
        + [device(dy=d) for d in (1, -1)]
        + [device(dk=1)]
    )
    barrier = pltpu.get_barrier_semaphore()
    for peer in peers:
        pl.semaphore_signal(barrier, inc=1, device_id=peer, device_id_type=MESH)

    wt[0] = gw[...].T
    wt[1] = lw[...].T
    for i in range(4):
        tst[i, 0:TB] = tok[i * TB : (i + 1) * TB]
        tst[i, TB : TB + GR] = jnp.broadcast_to(gain[...], (GR, DB))
    pl.semaphore_wait(barrier, len(peers))

    ids, sent = {}, []

    def copy_of(name, src, dst, to):
        i = ids.setdefault(name, len(ids))
        return pltpu.make_async_remote_copy(
            src_ref=src, dst_ref=dst, send_sem=send.at[i], recv_sem=recv.at[i],
            device_id=to, device_id_type=MESH,
        )

    def push(name, src, dst, to):
        copy = copy_of(name, src, dst, to)
        copy.start()
        sent.append(copy)

    def arrive(name, dst):
        copy_of(name, dst, dst, device(dk=1)).wait_recv()

    def token_block(dz):
        nz = wrap(z + dz, 8)
        return tks.at[lax.rem(nz, 2), k, lax.div(nz, 2)]

    def token_block_other(dz):
        nz = wrap(z + dz, 8)
        return tks.at[lax.rem(nz, 2), 1 - k, lax.div(nz, 2)]

    for e in (1, 3, 2):
        push(f"ta{4 - e}", tst.at[wrap(x + e, 4)], tks.at[zl, k, zh, x], device(dx=e))

    def rows_for(d):
        return pl.ds(pl.multiple_of(wrap(zh + d, 4) * FB, 16), FB)

    for e in (1, 3, 2):
        push(f"gz{4 - e}", wt.at[:, rows_for(e), :], gl.at[zh, y, :, x], device(dz=2 * e))
    for e in (1, 3, 2):
        push(f"wz{4 - e}", ow.at[rows_for(e), :], w2.at[zh, y, x], device(dz=2 * e))
    gl[zh, y, :, x] = wt[:, rows_for(0), :]
    w2[zh, y, x] = ow[rows_for(0), :]
    tks[zl, k, zh, x] = tst[x]

    class Unit:
        def __init__(self, kind, u, first, way):
            self.kind, self.u, self.first, self.way = kind, u, first, way
            self.tag = f"{kind}{first}{way}" if kind == "g" else f"{kind}{u}"
            self.p, self.q = (x, y) if first == "x" else (y, x)

        def block(self, df, ds):
            f, s = wrap(self.p + df, 4), wrap(self.q + ds, 4)
            yy, xx = (s, f) if self.first == "x" else (f, s)
            return gl.at[self.u, yy, :, xx] if self.kind == "g" else w2.at[self.u, yy, xx]

        def along(self, step, second=False):
            return device(dx=step) if (self.first == "x") != second else device(dy=step)

        def go(self, name, df, ds, step, second=False):
            ref = self.block(df, ds)
            push(f"{self.tag}{name}", ref, ref, self.along(step, second))

        def get(self, name, df, ds):
            arrive(f"{self.tag}{name}", self.block(df, ds))

        def spread(self, j):
            df = (0, -1, 1, 2)[j]
            self.go(f"L{j}", df, 0, 1, True)
            self.go(f"R{j}", df, 0, -1, True)

        def a0(self):
            self.go("l", 0, 0, 1)
            self.go("r", 0, 0, -1)
            self.spread(0)

        def a1(self):
            self.get("l", -1, 0)
            if self.way > 0:
                self.go("o", -1, 0, 1)
            self.spread(1)
            self.get("r", 1, 0)
            if self.way < 0:
                self.go("o", 1, 0, -1)
            self.spread(2)

        def a2(self):
            self.get("o", 2, 0)
            self.spread(3)

        def a3(self, j):
            df = (0, -1, 1, 2)[j]
            self.get(f"L{j}", df, -1)
            if j in (0, 3):
                self.go(f"O{j}", df, -1, 1, True)
            self.get(f"R{j}", df, 1)
            if j in (1, 2):
                self.go(f"O{j}", df, 1, -1, True)

        def a5(self):
            for j, df in enumerate((0, -1, 1, 2)):
                self.get(f"O{j}", df, 2)

    def each(units, stage, *args):
        for unit in units:
            getattr(unit, stage)(*args)

    def unit_of(d):
        return wrap(zh + d, 4)

    g0 = [Unit("g", unit_of(0), "x", 1), Unit("g", unit_of(1), "y", 1)]
    g1 = [Unit("g", unit_of(3), "x", -1), Unit("g", unit_of(2), "y", -1)]
    v0 = [Unit("w", 0, "x", 1), Unit("w", 2, "y", 1)]
    v1 = [Unit("w", 1, "x", -1), Unit("w", 3, "y", -1)]

    def z_arrival(name, d):
        u = unit_of(d)
        arrive(f"{name}{d}", gl.at[u, y, :, x] if name == "gz" else w2.at[u, y, x])

    def tokens_first():
        for d in (1, 3, 2):
            arrive(f"ta{d}", tks.at[zl, k, zh, wrap(x + d, 4)])
        own = token_block(0)
        push("tm1", own, own, device(dz=-1))
        push("tp1", own, own, device(dz=1))
        push("s0", own, own, device(dk=1))

    def tokens_next(m):
        block = token_block(m)
        arrive(f"tm{m}", block)
        if m < 4:
            push(f"tm{m + 1}", block, block, device(dz=-1))
        push(f"s{m}", block, block, device(dk=1))
        if m < 4:
            block = token_block(-m)
            arrive(f"tp{m}", block)
            if m < 3:
                push(f"tp{m + 1}", block, block, device(dz=1))
            push(f"s{-m}", block, block, device(dk=1))

    def tokens_last():
        for m in (0, 1, -1, 2, -2, 3, -3, 4):
            arrive(f"s{m}", token_block_other(m))

    def normalise():
        spots = [(a, b, c) for a in range(2) for b in range(2) for c in range(4)]

        @pl.loop(0, 4)
        def _(h):
            total = jnp.zeros((TB, DB), F32)
            for a, b, c in spots:
                v = tks[a, b, h, c, 0:TB, :].astype(F32)
                total = total + v * v
            mean = jnp.sum(total, axis=1, keepdims=True) * (1.0 / 4096.0)
            scale = lax.rsqrt(mean + 1e-06)
            rows = pl.ds(pl.multiple_of(h * TB, TB), TB)
            for a, b, c in spots:
                v = tks[a, b, h, c, 0:TB, :].astype(F32)
                g = tks[a, b, h, c, TB : TB + GR, :].astype(F32)[0:1, :]
                nrm[a * 8 + c * 2 + b, rows, :] = (v * scale * g).astype(BF)

    def project(unit, fresh=False):
        @pl.loop(0, 4)
        def _(t):
            left = nrm[unit.u * 4 + t]
            for a in range(2):
                term = lax.dot_general(
                    left, gl[unit.u, t, a].reshape(4 * FB, DB), NT, preferred_element_type=F32
                )
                acc[a] += term

    def activate():
        @pl.loop(0, 8)
        def _(t):
            rows = pl.ds(pl.multiple_of(t * 64, 64), 64)
            hid[rows, :] = (jax.nn.gelu(acc[0, rows, :], approximate=True) * acc[1, rows, :]).astype(BF)

    def terms(h, mine):
        core = k if mine else 1 - k

        @pl.loop(0, 4)
        def _(t):
            a, i = lax.div(t, 2), lax.rem(t, 2)
            right = w2[2 * a + h, 2 * i + core].reshape(4 * FB, DB)
            term = jnp.dot(hid[...], right, preferred_element_type=F32)
            if mine:
                part[h, a, i] = term
            else:
                stx[h, a, i] = term.astype(BF)

    def ring_value(h, dz):
        nz = wrap(z + dz, 8)
        a, rows = lax.rem(nz, 2), pl.ds(pl.multiple_of(lax.div(nz, 2) * TB, TB), TB)
        return part[h, a, :, rows, :] + srx[h, a, :, rows, :].astype(F32)

    def ring_step(h, s):
        for way in (0, 1):
            length = 4 if h == way else 3
            if s >= length:
                continue
            sign = 1 if way == 0 else -1
            value = ring_value(h, sign * (length - s))
            if s > 0:
                arrive(f"r{h}{way}{s - 1}", rrx.at[h, way, s - 1])
                value = value + rrx[h, way, s - 1].astype(F32)
            rtx[h, way, s] = value.astype(BF)
            push(f"r{h}{way}{s}", rtx.at[h, way, s], rrx.at[h, way, s], device(dz=sign))

    def ring_end(h):
        value = ring_value(h, 0)
        for way in (0, 1):
            last = 3 if h == way else 2
            arrive(f"r{h}{way}{last}", rrx.at[h, way, last])
            value = value + rrx[h, way, last].astype(F32)
        fin[2 * h : 2 * h + 2] = value.astype(BF)

    def sum_first(h):
        terms(h, False)
        push(f"c{h}", stx.at[h], srx.at[h], device(dk=1))
        terms(h, True)
        arrive(f"c{h}", srx.at[h])

    each(g0[:1], "a0")
    acc[...] = jnp.zeros_like(acc)
    tokens_first()
    z_arrival("gz", 1)
    each(g0[1:], "a0")
    each(g0, "a1")
    tokens_next(1)
    each(g0, "a2")
    each(g0, "a3", 0)
    each(g0, "a3", 1)
    tokens_next(2)
    z_arrival("gz", 3)
    z_arrival("gz", 2)
    each(g1, "a0")
    each(g0, "a3", 2)
    each(g0, "a3", 3)
    tokens_next(3)
    each(g1, "a1")
    each(g1, "a2")
    tokens_next(4)
    each(g0, "a5")
    for d in (1, 3, 2):
        z_arrival("wz", d)
    each(g1, "a3", 0)
    each(v0, "a0")
    tokens_last()
    normalise()
    each(g1, "a3", 1)
    each(g1, "a3", 2)
    project(g0[0])
    each(g1, "a3", 3)
    project(g0[1])
    each(v0, "a1")
    each(v0, "a2")
    each(v1, "a0")
    each(g1, "a5")
    project(g1[0])
    each(v0, "a3", 0)
    each(v0, "a3", 1)
    project(g1[1])
    each(v0, "a3", 2)
    each(v0, "a3", 3)
    each(v1, "a1")
    each(v1, "a2")
    activate()
    each(v0, "a5")
    sum_first(0)
    ring_step(0, 0)
    each(v1, "a3", 0)
    each(v1, "a3", 1)
    ring_step(0, 1)
    each(v1, "a3", 2)
    each(v1, "a3", 3)
    ring_step(0, 2)
    each(v1, "a5")
    sum_first(1)
    ring_step(1, 0)
    ring_step(0, 3)
    ring_step(1, 1)
    ring_end(0)
    ring_step(1, 2)
    ring_step(1, 3)
    ring_end(1)
    for e in (1, 3, 2):
        push(f"f{4 - e}", fin.at[wrap(x + e, 4)], land.at[x], device(dx=e))
    land[x] = fin[x]
    for d in (1, 3, 2):
        arrive(f"f{d}", land.at[wrap(x + d, 4)])
    out[...] = land[...].reshape(4 * TB, DB)
    for copy in sent:
        copy.wait_send()
    assert len(ids) <= N_SEMS, len(ids)


def local(tokens, norm_gain, gate_weight, linear_weight, output_weight):
    vmem = pl.BlockSpec(memory_space=pltpu.VMEM)
    return pl.pallas_call(
        kernel,
        out_shape=jax.ShapeDtypeStruct((4 * TB, DB), BF),
        in_specs=[vmem] * 5,
        out_specs=vmem,
        scratch_shapes=[
            pltpu.VMEM((2, 4 * FB, DB), BF),
            pltpu.VMEM((4, 4, 2, 4, FB, DB), BF),
            pltpu.VMEM((4, 4, 4, FB, DB), BF),
            pltpu.VMEM((4, TB + GR, DB), BF),
            pltpu.VMEM((2, 2, 4, 4, TB + GR, DB), BF),
            pltpu.VMEM((16, 4 * TB, DB), BF),
            pltpu.VMEM((2, 4 * TB, 4 * FB), F32),
            pltpu.VMEM((4 * TB, 4 * FB), BF),
            pltpu.VMEM((2, 2, 2, 4 * TB, DB), F32),
            pltpu.VMEM((2, 2, 2, 4 * TB, DB), BF),
            pltpu.VMEM((2, 2, 2, 4 * TB, DB), BF),
            pltpu.VMEM((2, 2, 4, 2, TB, DB), BF),
            pltpu.VMEM((2, 2, 4, 2, TB, DB), BF),
            pltpu.VMEM((4, TB, DB), BF),
            pltpu.VMEM((4, TB, DB), BF),
            pltpu.SemaphoreType.DMA((N_SEMS,)),
            pltpu.SemaphoreType.DMA((N_SEMS,)),
        ],
        compiler_params=pltpu.CompilerParams(
            collective_id=0, has_side_effects=True, vmem_limit_bytes=60 * 1024 * 1024
        ),
    )(tokens, norm_gain.reshape(1, DB), gate_weight, linear_weight, output_weight)


def solution(mesh):
    return jax.shard_map(
        local,
        mesh=mesh,
        in_specs=(P("row", "col"), P("col"), P("row", "col"), P("row", "col"), P("col", "row")),
        out_specs=P("row", "col"),
        check_vma=False,
    )
```

```python
import jax
import jax.numpy as jnp
from jax import lax
from jax.experimental import pallas as pl
from jax.experimental.pallas import tpu as pltpu
from jax.sharding import PartitionSpec as P

MESH = pl.DeviceIdType.MESH
BF, F32 = jnp.bfloat16, jnp.float32
FB = 160
DB = 256
HB = DB // 2
TB = 128
GR = 16
N_SEMS = 320
NT = (((1,), (1,)), ((), ()))


def wrap(v, n):
    return lax.rem(v + n, n)


def kernel(
    tok, gain, gw, lw, ow, out,
    wt, gl, w2, tst, tks, nrm, acc, hid, part, stx, srx, rtx, rrx, fin, land, send, recv,
):
    row, col = lax.axis_index("row"), lax.axis_index("col")
    zh, y = lax.div(row, 4), lax.rem(row, 4)
    zl, x, k = lax.div(col, 8), lax.rem(lax.div(col, 2), 4), lax.rem(col, 2)
    z = zh * 2 + zl

    def device(dz=0, dy=0, dx=0, dk=0):
        nz, ny, nx = wrap(z + dz, 8), wrap(y + dy, 4), wrap(x + dx, 4)
        return (lax.div(nz, 2) * 4 + ny, lax.rem(nz, 2) * 8 + nx * 2 + lax.rem(k + dk, 2))

    peers = (
        [device(dz=d) for d in (1, -1, 2, -2, 4)]
        + [device(dx=d) for d in (1, -1, 2)]
        + [device(dy=d) for d in (1, -1)]
        + [device(dk=1)]
    )
    barrier = pltpu.get_barrier_semaphore()
    for peer in peers:
        pl.semaphore_signal(barrier, inc=1, device_id=peer, device_id_type=MESH)

    wt[0] = gw[...].T
    wt[1] = lw[...].T
    for i in range(4):
        tst[i, 0:TB] = tok[i * TB : (i + 1) * TB]
        tst[i, TB : TB + GR] = jnp.broadcast_to(gain[...], (GR, DB))
    pl.semaphore_wait(barrier, len(peers))

    ids, sent = {}, []

    def copy_of(name, src, dst, to):
        i = ids.setdefault(name, len(ids))
        return pltpu.make_async_remote_copy(
            src_ref=src, dst_ref=dst, send_sem=send.at[i], recv_sem=recv.at[i],
            device_id=to, device_id_type=MESH,
        )

    def push(name, src, dst, to):
        copy = copy_of(name, src, dst, to)
        copy.start()
        sent.append(copy)

    def arrive(name, dst):
        copy_of(name, dst, dst, device(dk=1)).wait_recv()

    def token_block(dz):
        nz = wrap(z + dz, 8)
        return tks.at[lax.rem(nz, 2), k, lax.div(nz, 2)]

    def token_block_other(dz):
        nz = wrap(z + dz, 8)
        return tks.at[lax.rem(nz, 2), 1 - k, lax.div(nz, 2)]

    for e in (1, 3, 2):
        push(f"ta{4 - e}", tst.at[wrap(x + e, 4)], tks.at[zl, k, zh, x], device(dx=e))

    def rows_for(d):
        return pl.ds(pl.multiple_of(wrap(zh + d, 4) * FB, 16), FB)

    for e in (1, 3, 2):
        push(f"gz{4 - e}", wt.at[:, rows_for(e), :], gl.at[zh, y, :, x], device(dz=2 * e))
    for e in (1, 3, 2):
        for c in range(2):
            half = pl.ds(c * HB, HB)
            push(f"wz{c}{4 - e}", ow.at[rows_for(e), half], w2.at[c, zh, y, x], device(dz=2 * e))
    gl[zh, y, :, x] = wt[:, rows_for(0), :]
    for c in range(2):
        w2[c, zh, y, x] = ow[rows_for(0), c * HB : (c + 1) * HB]
    tks[zl, k, zh, x] = tst[x]

    class Unit:
        def __init__(self, kind, u, tag, first, way):
            self.kind, self.u, self.first, self.way = kind, u, first, way
            self.tag = f"k{kind}{tag}"
            self.p, self.q = (x, y) if first == "x" else (y, x)

        def block(self, df, ds):
            f, s = wrap(self.p + df, 4), wrap(self.q + ds, 4)
            yy, xx = (s, f) if self.first == "x" else (f, s)
            if self.kind < 2:
                return gl.at[self.u, yy, self.kind, xx]
            return w2.at[self.kind - 2, self.u, yy, xx]

        def along(self, step, second=False):
            return device(dx=step) if (self.first == "x") != second else device(dy=step)

        def go(self, name, df, ds, step, second=False):
            ref = self.block(df, ds)
            push(f"{self.tag}{name}", ref, ref, self.along(step, second))

        def get(self, name, df, ds):
            arrive(f"{self.tag}{name}", self.block(df, ds))

        def spread(self, j):
            df = (0, -1, 1, 2)[j]
            self.go(f"L{j}", df, 0, 1, True)
            self.go(f"R{j}", df, 0, -1, True)

        def a0(self):
            self.go("l", 0, 0, 1)
            self.go("r", 0, 0, -1)
            self.spread(0)

        def a1(self):
            self.get("l", -1, 0)
            if self.way > 0:
                self.go("o", -1, 0, 1)
            self.spread(1)
            self.get("r", 1, 0)
            if self.way < 0:
                self.go("o", 1, 0, -1)
            self.spread(2)

        def a2(self):
            self.get("o", 2, 0)
            self.spread(3)

        def a3(self, j):
            df = (0, -1, 1, 2)[j]
            self.get(f"L{j}", df, -1)
            if j in (0, 3):
                self.go(f"O{j}", df, -1, 1, True)
            self.get(f"R{j}", df, 1)
            if j in (1, 2):
                self.go(f"O{j}", df, 1, -1, True)

        def a5(self):
            for j, df in enumerate((0, -1, 1, 2)):
                self.get(f"O{j}", df, 2)

    def each(units, stage, *args):
        for unit in units:
            getattr(unit, stage)(*args)

    def unit_of(d):
        return wrap(zh + d, 4)

    def pair(n, d):
        way = 1 if n % 2 == 0 else -1
        return [Unit(0, unit_of(d), d, "x", way), Unit(1, unit_of(d), d, "y", way)]

    g = [pair(n, d) for n, d in enumerate((0, 1, 3, 2))]
    v = [
        [
            [Unit(2 + c, h, h, "x", 1 - 2 * h), Unit(2 + c, 2 + h, 2 + h, "y", 1 - 2 * h)]
            for h in range(2)
        ]
        for c in range(2)
    ]

    def weights_in(d):
        arrive(f"gz{d}", gl.at[unit_of(d), y, :, x])

    def outputs_in(c):
        for d in (1, 3, 2):
            arrive(f"wz{c}{d}", w2.at[c, unit_of(d), y, x])

    def tokens_first():
        for d in (1, 3, 2):
            arrive(f"ta{d}", tks.at[zl, k, zh, wrap(x + d, 4)])
        own = token_block(0)
        push("tm1", own, own, device(dz=-1))
        push("tp1", own, own, device(dz=1))
        push("s0", own, own, device(dk=1))

    def tokens_next(m):
        block = token_block(m)
        arrive(f"tm{m}", block)
        if m < 4:
            push(f"tm{m + 1}", block, block, device(dz=-1))
        push(f"s{m}", block, block, device(dk=1))
        if m < 4:
            block = token_block(-m)
            arrive(f"tp{m}", block)
            if m < 3:
                push(f"tp{m + 1}", block, block, device(dz=1))
            push(f"s{-m}", block, block, device(dk=1))

    def tokens_last():
        for m in (0, 1, -1, 2, -2, 3, -3, 4):
            arrive(f"s{m}", token_block_other(m))

    def normalise():
        spots = [(a, b, c) for a in range(2) for b in range(2) for c in range(4)]

        @pl.loop(0, 4)
        def _(h):
            total = jnp.zeros((TB, DB), F32)
            for a, b, c in spots:
                v = tks[a, b, h, c, 0:TB, :].astype(F32)
                total = total + v * v
            mean = jnp.sum(total, axis=1, keepdims=True) * (1.0 / 4096.0)
            scale = lax.rsqrt(mean + 1e-06)
            rows = pl.ds(pl.multiple_of(h * TB, TB), TB)
            for a, b, c in spots:
                v = tks[a, b, h, c, 0:TB, :].astype(F32)
                g = tks[a, b, h, c, TB : TB + GR, :].astype(F32)[0:1, :]
                nrm[a * 8 + c * 2 + b, rows, :] = (v * scale * g).astype(BF)

    def project(n):
        u = g[n][0].u

        @pl.loop(0, 4)
        def _(t):
            left = nrm[u * 4 + t]
            for a in range(2):
                right = gl[u, t, a].reshape(4 * FB, DB)
                acc[a] += lax.dot_general(left, right, NT, preferred_element_type=F32)

    def activate():
        @pl.loop(0, 8)
        def _(t):
            rows = pl.ds(pl.multiple_of(t * 64, 64), 64)
            hid[rows, :] = (jax.nn.gelu(acc[0, rows, :], approximate=True) * acc[1, rows, :]).astype(BF)

    def terms(c, mine):
        core = k if mine else 1 - k

        @pl.loop(0, 4)
        def _(t):
            h, a = lax.div(t, 2), lax.rem(t, 2)
            blocks = [w2[c, 2 * a + h, 2 * i + core].reshape(4 * FB, HB) for i in range(2)]
            right = jnp.concatenate(blocks, axis=1)
            term = jnp.dot(hid[...], right, preferred_element_type=F32)
            if mine:
                part[c, h, a] = term
            else:
                stx[c, h, a] = term.astype(BF)

    def ring_value(c, h, dz):
        nz = wrap(z + dz, 8)
        a, rows = lax.rem(nz, 2), pl.ds(pl.multiple_of(lax.div(nz, 2) * TB, TB), TB)
        return part[c, h, a, rows, :] + srx[c, h, a, rows, :].astype(F32)

    def ring_step(c, s):
        for h in (0, 1):
            for way in (0, 1):
                length = 4 if h == way else 3
                if s >= length:
                    continue
                sign = 1 if way == 0 else -1
                value = ring_value(c, h, sign * (length - s))
                if s > 0:
                    arrive(f"r{c}{h}{way}{s - 1}", rrx.at[c, h, way, s - 1])
                    value = value + rrx[c, h, way, s - 1].astype(F32)
                rtx[c, h, way, s] = value.astype(BF)
                push(f"r{c}{h}{way}{s}", rtx.at[c, h, way, s], rrx.at[c, h, way, s], device(dz=sign))

    def ring_end(c):
        for h in (0, 1):
            value = ring_value(c, h, 0)
            for way in (0, 1):
                last = 3 if h == way else 2
                arrive(f"r{c}{h}{way}{last}", rrx.at[c, h, way, last])
                value = value + rrx[c, h, way, last].astype(F32)
            for i in range(2):
                fin[c, 2 * h + i] = value[:, i * HB : (i + 1) * HB].astype(BF)
        for e in (1, 3, 2):
            push(f"f{c}{4 - e}", fin.at[c, wrap(x + e, 4)], land.at[c, x], device(dx=e))
        land[c, x] = fin[c, x]

    def finish(c):
        for d in (1, 3, 2):
            arrive(f"f{c}{d}", land.at[c, wrap(x + d, 4)])
        out[:, c * HB : (c + 1) * HB] = land[c].reshape(4 * TB, HB)

    def sum_first(c):
        terms(c, False)
        push(f"c{c}", stx.at[c], srx.at[c], device(dk=1))
        terms(c, True)
        arrive(f"c{c}", srx.at[c])

    def reach(units, *js):
        for j in js:
            each(units, "a3", j)

    each(g[0], "a0")
    acc[...] = jnp.zeros_like(acc)
    tokens_first()
    each(g[0], "a1")
    each(g[0], "a2")
    weights_in(1)
    each(g[1], "a0")
    reach(g[0], 0, 1)
    tokens_next(1)
    each(g[1], "a1")
    reach(g[0], 2, 3)
    each(g[1], "a2")
    weights_in(3)
    each(g[2], "a0")
    tokens_next(2)
    each(g[0], "a5")
    reach(g[1], 0, 1)
    each(g[2], "a1")
    reach(g[1], 2, 3)
    each(g[2], "a2")
    tokens_next(3)
    weights_in(2)
    each(g[3], "a0")
    each(g[1], "a5")
    reach(g[2], 0, 1)
    tokens_next(4)
    each(g[3], "a1")
    reach(g[2], 2, 3)
    each(g[3], "a2")
    outputs_in(0)
    each(v[0][0], "a0")
    each(g[2], "a5")
    tokens_last()
    normalise()
    reach(g[3], 0, 1)
    each(v[0][0], "a1")
    project(0)
    reach(g[3], 2, 3)
    each(v[0][0], "a2")
    each(v[0][1], "a0")
    project(1)
    each(g[3], "a5")
    reach(v[0][0], 0, 1)
    each(v[0][1], "a1")
    project(2)
    reach(v[0][0], 2, 3)
    each(v[0][1], "a2")
    outputs_in(1)
    each(v[1][0], "a0")
    project(3)
    each(v[0][0], "a5")
    reach(v[0][1], 0, 1)
    each(v[1][0], "a1")
    activate()
    reach(v[0][1], 2, 3)
    each(v[1][0], "a2")
    each(v[1][1], "a0")
    each(v[0][1], "a5")
    sum_first(0)
    ring_step(0, 0)
    reach(v[1][0], 0, 1, 2, 3)
    each(v[1][1], "a1")
    each(v[1][1], "a2")
    ring_step(0, 1)
    each(v[1][0], "a5")
    reach(v[1][1], 0, 1)
    ring_step(0, 2)
    reach(v[1][1], 2, 3)
    ring_step(0, 3)
    each(v[1][1], "a5")
    sum_first(1)
    ring_step(1, 0)
    ring_end(0)
    ring_step(1, 1)
    ring_step(1, 2)
    ring_step(1, 3)
    ring_end(1)
    finish(0)
    finish(1)
    for copy in sent:
        copy.wait_send()
    assert len(ids) <= N_SEMS, len(ids)


def local(tokens, norm_gain, gate_weight, linear_weight, output_weight):
    vmem = pl.BlockSpec(memory_space=pltpu.VMEM)
    return pl.pallas_call(
        kernel,
        out_shape=jax.ShapeDtypeStruct((4 * TB, DB), BF),
        in_specs=[vmem] * 5,
        out_specs=vmem,
        scratch_shapes=[
            pltpu.VMEM((2, 4 * FB, DB), BF),
            pltpu.VMEM((4, 4, 2, 4, FB, DB), BF),
            pltpu.VMEM((2, 4, 4, 4, FB, HB), BF),
            pltpu.VMEM((4, TB + GR, DB), BF),
            pltpu.VMEM((2, 2, 4, 4, TB + GR, DB), BF),
            pltpu.VMEM((16, 4 * TB, DB), BF),
            pltpu.VMEM((2, 4 * TB, 4 * FB), F32),
            pltpu.VMEM((4 * TB, 4 * FB), BF),
            pltpu.VMEM((2, 2, 2, 4 * TB, DB), F32),
            pltpu.VMEM((2, 2, 2, 4 * TB, DB), BF),
            pltpu.VMEM((2, 2, 2, 4 * TB, DB), BF),
            pltpu.VMEM((2, 2, 2, 4, TB, DB), BF),
            pltpu.VMEM((2, 2, 2, 4, TB, DB), BF),
            pltpu.VMEM((2, 4, TB, HB), BF),
            pltpu.VMEM((2, 4, TB, HB), BF),
            pltpu.SemaphoreType.DMA((N_SEMS,)),
            pltpu.SemaphoreType.DMA((N_SEMS,)),
        ],
        compiler_params=pltpu.CompilerParams(
            collective_id=0, has_side_effects=True, vmem_limit_bytes=60 * 1024 * 1024
        ),
    )(tokens, norm_gain.reshape(1, DB), gate_weight, linear_weight, output_weight)


def solution(mesh):
    return jax.shard_map(
        local,
        mesh=mesh,
        in_specs=(P("row", "col"), P("col"), P("row", "col"), P("row", "col"), P("col", "row")),
        out_specs=P("row", "col"),
        check_vma=False,
    )
```

```python
import jax
import jax.numpy as jnp
from jax import lax
from jax.experimental import pallas as pl
from jax.experimental.pallas import tpu as pltpu
from jax.sharding import PartitionSpec as P

MESH = pl.DeviceIdType.MESH
BF, F32 = jnp.bfloat16, jnp.float32
FB = 160
DB = 256
HB = DB // 2
TB = 128
GR = 16
N_SEMS = 320
NT = (((1,), (1,)), ((), ()))


def wrap(v, n):
    return lax.rem(v + n, n)


def kernel(
    tok, gain, gw, lw, ow, out,
    wt, gl, w2, tst, tks, nrm, acc, hid, part, stx, srx, rtx, rrx, fin, land, send, recv,
):
    row, col = lax.axis_index("row"), lax.axis_index("col")
    zh, y = lax.div(row, 4), lax.rem(row, 4)
    zl, x, k = lax.div(col, 8), lax.rem(lax.div(col, 2), 4), lax.rem(col, 2)
    z = zh * 2 + zl

    def device(dz=0, dy=0, dx=0, dk=0):
        nz, ny, nx = wrap(z + dz, 8), wrap(y + dy, 4), wrap(x + dx, 4)
        return (lax.div(nz, 2) * 4 + ny, lax.rem(nz, 2) * 8 + nx * 2 + lax.rem(k + dk, 2))

    peers = (
        [device(dz=d) for d in (1, -1, 2, -2, 4)]
        + [device(dx=d) for d in (1, -1, 2)]
        + [device(dy=d) for d in (1, -1)]
        + [device(dk=1)]
    )
    barrier = pltpu.get_barrier_semaphore()
    for peer in peers:
        pl.semaphore_signal(barrier, inc=1, device_id=peer, device_id_type=MESH)

    wt[0] = gw[...].T
    wt[1] = lw[...].T
    for i in range(4):
        tst[i, 0:TB] = tok[i * TB : (i + 1) * TB]
        tst[i, TB : TB + GR] = jnp.broadcast_to(gain[...], (GR, DB))
    pl.semaphore_wait(barrier, len(peers))

    ids, sent = {}, []

    def copy_of(name, src, dst, to):
        i = ids.setdefault(name, len(ids))
        return pltpu.make_async_remote_copy(
            src_ref=src, dst_ref=dst, send_sem=send.at[i], recv_sem=recv.at[i],
            device_id=to, device_id_type=MESH,
        )

    def push(name, src, dst, to):
        copy = copy_of(name, src, dst, to)
        copy.start()
        sent.append(copy)

    def arrive(name, dst):
        copy_of(name, dst, dst, device(dk=1)).wait_recv()

    def token_block(dz):
        nz = wrap(z + dz, 8)
        return tks.at[lax.rem(nz, 2), k, lax.div(nz, 2)]

    def token_block_other(dz):
        nz = wrap(z + dz, 8)
        return tks.at[lax.rem(nz, 2), 1 - k, lax.div(nz, 2)]

    for e in (1, 3, 2):
        push(("ta", 4 - e), tst.at[wrap(x + e, 4)], tks.at[zl, k, zh, x], device(dx=e))

    def rows_for(d):
        return pl.ds(pl.multiple_of(wrap(zh + d, 4) * FB, 16), FB)

    def exchange_inputs(e):
        push(("gz", 4 - e), wt.at[:, rows_for(e), :], gl.at[zh, y, :, x], device(dz=2 * e))

    def exchange_outputs():
        for c in range(2):
            for e in (1, 3, 2):
                half = pl.ds(c * HB, HB)
                push(("wz", c, 4 - e), ow.at[rows_for(e), half], w2.at[c, zh, y, x], device(dz=2 * e))

    exchange_inputs(1)
    exchange_inputs(3)
    gl[zh, y, :, x] = wt[:, rows_for(0), :]
    for c in range(2):
        w2[c, zh, y, x] = ow[rows_for(0), c * HB : (c + 1) * HB]
    tks[zl, k, zh, x] = tst[x]

    class Unit:
        def __init__(self, kind, u, tag, first, way):
            self.kind, self.u, self.first, self.way = kind, u, first, way
            self.tag = (kind, tag)
            self.p, self.q = (x, y) if first == "x" else (y, x)

        def block(self, df, ds):
            f, s = wrap(self.p + df, 4), wrap(self.q + ds, 4)
            yy, xx = (s, f) if self.first == "x" else (f, s)
            if self.kind < 2:
                return gl.at[self.u, yy, self.kind, xx]
            return w2.at[self.kind - 2, self.u, yy, xx]

        def along(self, step, second=False):
            return device(dx=step) if (self.first == "x") != second else device(dy=step)

        def go(self, name, j, df, ds, step, second=False):
            ref = self.block(df, ds)
            push((self.tag, name, j), ref, ref, self.along(step, second))

        def get(self, name, j, df, ds):
            arrive((self.tag, name, j), self.block(df, ds))

        def spread(self, j):
            df = (0, -1, 1, 2)[j]
            self.go("L", j, df, 0, 1, True)
            self.go("R", j, df, 0, -1, True)

        def a0(self):
            self.go("l", 0, 0, 0, 1)
            self.go("r", 0, 0, 0, -1)
            self.spread(0)

        def a1l(self):
            self.get("l", 0, -1, 0)
            if self.way > 0:
                self.go("o", 0, -1, 0, 1)
            self.spread(1)

        def a1r(self):
            self.get("r", 0, 1, 0)
            if self.way < 0:
                self.go("o", 0, 1, 0, -1)
            self.spread(2)

        def a2(self):
            self.get("o", 0, 2, 0)
            self.spread(3)

        def b(self, j):
            df = (0, -1, 1, 2)[j]
            if j in (0, 3):
                self.get("L", j, df, -1)
                self.go("O", j, df, -1, 1, True)
            else:
                self.get("R", j, df, 1)
                self.go("O", j, df, 1, -1, True)

        def end(self):
            for j, df in enumerate((0, -1, 1, 2)):
                if j in (0, 3):
                    self.get("R", j, df, 1)
                else:
                    self.get("L", j, df, -1)
                self.get("O", j, df, 2)

    def unit_of(d):
        return wrap(zh + d, 4)

    def pair(n, d):
        way = 1 if n % 2 == 0 else -1
        return [Unit(0, unit_of(d), d, "x", way), Unit(1, unit_of(d), d, "y", way)]

    g = [pair(n, d) for n, d in enumerate((0, 1, 3, 2))]
    v = [
        [
            [Unit(2 + c, h, h, "x", 1 - 2 * h), Unit(2 + c, 2 + h, 2 + h, "y", 1 - 2 * h)]
            for h in range(2)
        ]
        for c in range(2)
    ]

    def weights_in(d):
        arrive(("gz", d), gl.at[unit_of(d), y, :, x])

    def outputs_in(c):
        for d in (1, 3, 2):
            arrive(("wz", c, d), w2.at[c, unit_of(d), y, x])

    def tokens_first():
        for d in (1, 3, 2):
            arrive(("ta", d), tks.at[zl, k, zh, wrap(x + d, 4)])
        own = token_block(0)
        push(("tm", 1), own, own, device(dz=-1))
        push(("tp", 1), own, own, device(dz=1))
        push(("s", 0), own, own, device(dk=1))
        exchange_inputs(2)

    def tokens_down(m):
        block = token_block(m)
        arrive(("tm", m), block)
        if m < 4:
            push(("tm", m + 1), block, block, device(dz=-1))
        push(("s", m), block, block, device(dk=1))

    def tokens_up(m):
        block = token_block(-m)
        arrive(("tp", m), block)
        if m < 3:
            push(("tp", m + 1), block, block, device(dz=1))
        push(("s", -m), block, block, device(dk=1))
        if m == 2:
            exchange_outputs()

    def tokens_last():
        for m in (0, 1, -1, 2, -2, 3, -3, 4):
            arrive(("s", m), token_block_other(m))

    def normalise(h):
        spots = [(a, b, c) for a in range(2) for b in range(2) for c in range(4)]

        total = jnp.zeros((TB, DB), F32)
        for a, b, c in spots:
            v = tks[a, b, h, c, 0:TB, :].astype(F32)
            total = total + v * v
        mean = jnp.sum(total, axis=1, keepdims=True) * (1.0 / 4096.0)
        scale = lax.rsqrt(mean + 1e-06)
        for a, b, c in spots:
            v = tks[a, b, h, c, 0:TB, :].astype(F32)
            g = tks[a, b, h, c, TB : TB + GR, :].astype(F32)[0:1, :]
            nrm[a * 8 + c * 2 + b, h * TB : (h + 1) * TB, :] = (v * scale * g).astype(BF)

    def project(n, t):
        u = g[n][0].u
        for a in range(2):
            right = gl[u, t, a].reshape(4 * FB, DB)
            acc[a] += lax.dot_general(nrm[u * 4 + t], right, NT, preferred_element_type=F32)

    def activate(q):
        @pl.loop(2 * q, 2 * q + 2)
        def _(t):
            rows = pl.ds(pl.multiple_of(t * 64, 64), 64)
            hid[rows, :] = (jax.nn.gelu(acc[0, rows, :], approximate=True) * acc[1, rows, :]).astype(BF)

    def terms(c, h, mine):
        core = k if mine else 1 - k

        @pl.loop(0, 2)
        def _(a):
            blocks = [w2[c, 2 * a + h, 2 * i + core].reshape(4 * FB, HB) for i in range(2)]
            right = jnp.concatenate(blocks, axis=1)
            term = jnp.dot(hid[...], right, preferred_element_type=F32)
            if mine:
                part[c, h, a] = term
            else:
                stx[c, h, a] = term.astype(BF)

        if not mine:
            push(("c", c, h), stx.at[c, h], srx.at[c, h], device(dk=1))

    def ring_value(c, h, dz):
        nz = wrap(z + dz, 8)
        a, rows = lax.rem(nz, 2), pl.ds(pl.multiple_of(lax.div(nz, 2) * TB, TB), TB)
        return part[c, h, a, rows, :] + srx[c, h, a, rows, :].astype(F32)

    def ring_step(c, h, s):
        if s == 0:
            arrive(("c", c, h), srx.at[c, h])
        for way in (0, 1):
            length = 4 if h == way else 3
            if s >= length:
                continue
            sign = 1 if way == 0 else -1
            value = ring_value(c, h, sign * (length - s))
            if s > 0:
                arrive(("r", c, h, way, s - 1), rrx.at[c, h, way, s - 1])
                value = value + rrx[c, h, way, s - 1].astype(F32)
            rtx[c, h, way, s] = value.astype(BF)
            push(("r", c, h, way, s), rtx.at[c, h, way, s], rrx.at[c, h, way, s], device(dz=sign))

    def ring_end(c, h):
        value = ring_value(c, h, 0)
        for way in (0, 1):
            last = 3 if h == way else 2
            arrive(("r", c, h, way, last), rrx.at[c, h, way, last])
            value = value + rrx[c, h, way, last].astype(F32)
        for i in range(2):
            fin[c, 2 * h + i] = value[:, i * HB : (i + 1) * HB].astype(BF)

    def hand_over(c):
        for e in (1, 3, 2):
            push(("f", c, 4 - e), fin.at[c, wrap(x + e, 4)], land.at[c, x], device(dx=e))
        land[c, x] = fin[c, x]

    def finish(c):
        for d in (1, 3, 2):
            arrive(("f", c, d), land.at[c, wrap(x + d, 4)])
        out[:, c * HB : (c + 1) * HB] = land[c].reshape(4 * TB, HB)

    acc[...] = jnp.zeros_like(acc)
    g[0][0].a0()
    g[0][1].a0()
    g[0][0].b(0)
    g[0][0].a1r()
    g[0][1].a1l()
    g[0][1].a1r()
    tokens_first()
    g[0][0].a1l()
    g[0][0].b(2)
    g[0][1].b(1)
    weights_in(3)
    weights_in(1)
    g[1][0].a0()
    g[1][1].a0()
    g[0][1].b(0)
    g[0][1].a2()
    g[0][1].b(2)
    g[0][0].b(1)
    g[1][0].b(0)
    g[1][0].a1r()
    g[0][0].a2()
    tokens_down(1)
    tokens_up(1)
    g[1][1].a1l()
    g[1][0].a1l()
    g[1][1].a1r()
    g[2][0].a0()
    g[1][1].b(0)
    g[2][1].a0()
    g[1][0].b(2)
    g[0][0].b(3)
    g[1][0].a2()
    g[0][1].b(3)
    g[1][1].b(1)
    tokens_down(2)
    g[1][0].b(1)
    g[2][0].b(0)
    g[1][1].b(2)
    g[1][1].a2()
    g[2][1].a1l()
    g[2][0].a1r()
    g[2][0].a1l()
    g[0][0].end()
    g[2][1].a1r()
    g[1][0].b(3)
    g[2][1].b(0)
    weights_in(2)
    tokens_down(3)
    g[3][0].a0()
    g[0][1].end()
    g[2][1].a2()
    g[1][1].b(3)
    g[3][1].a0()
    g[2][1].b(1)
    tokens_up(2)
    g[2][0].b(2)
    g[2][1].b(2)
    g[2][0].a2()
    g[2][0].b(1)
    g[1][0].end()
    g[3][0].a1r()
    tokens_down(4)
    g[3][0].b(0)
    g[3][1].a1r()
    g[3][1].a1l()
    g[3][0].a1l()
    tokens_up(3)
    g[2][0].b(3)
    g[2][1].b(3)
    tokens_last()
    normalise(0)
    normalise(1)
    g[3][0].a2()
    normalise(2)
    g[3][0].b(2)
    g[3][1].b(0)
    normalise(3)
    g[3][1].b(2)
    project(0, 0)
    g[3][1].a2()
    project(0, 1)
    outputs_in(0)
    g[3][1].b(1)
    v[0][0][0].a0()
    v[0][0][1].a0()
    project(0, 2)
    g[3][0].b(1)
    project(0, 3)
    g[1][1].end()
    g[3][0].b(3)
    project(1, 0)
    project(1, 1)
    project(1, 2)
    v[0][0][0].b(0)
    project(1, 3)
    v[0][0][1].a1l()
    g[2][0].end()
    g[2][1].end()
    project(2, 0)
    outputs_in(1)
    project(2, 1)
    g[3][1].b(3)
    v[0][0][1].a1r()
    project(2, 2)
    v[0][0][0].a1l()
    v[0][0][0].a1r()
    v[0][1][0].a0()
    v[0][1][1].a0()
    project(2, 3)
    v[0][0][1].a2()
    v[0][0][1].b(0)
    g[3][0].end()
    v[0][0][1].b(1)
    v[0][0][1].b(2)
    v[0][0][0].b(1)
    g[3][1].end()
    v[0][0][0].b(2)
    v[0][1][0].a1r()
    project(3, 0)
    project(3, 1)
    v[0][1][0].b(0)
    project(3, 2)
    v[0][0][0].a2()
    v[0][1][1].a1l()
    v[0][1][1].a1r()
    v[1][0][0].a0()
    v[0][1][0].a1l()
    v[1][0][1].a0()
    project(3, 3)
    activate(0)
    v[0][1][1].b(0)
    activate(1)
    v[0][0][1].b(3)
    v[0][1][0].a2()
    activate(2)
    v[0][1][0].b(2)
    activate(3)
    v[0][0][0].b(3)
    v[0][1][1].b(1)
    v[1][0][0].b(0)
    v[0][1][1].b(2)
    v[0][1][1].a2()
    v[1][0][0].a1r()
    v[1][0][1].a1l()
    v[1][0][0].a1l()
    v[0][1][0].b(1)
    v[0][1][0].b(3)
    v[1][0][1].b(0)
    v[1][0][1].a1r()
    v[1][1][0].a0()
    v[1][1][1].a0()
    v[0][0][0].end()
    v[0][0][1].end()
    terms(0, 0, False)
    v[0][1][1].b(3)
    terms(0, 0, True)
    v[1][0][0].b(2)
    v[1][0][1].b(1)
    v[1][0][1].a2()
    v[1][0][1].b(2)
    v[1][0][0].b(1)
    v[1][0][0].a2()
    v[1][1][0].a1r()
    ring_step(0, 0, 0)
    v[0][1][0].end()
    v[1][1][0].b(0)
    v[1][1][1].a1r()
    v[1][1][1].a1l()
    v[1][1][0].a1l()
    v[1][0][0].b(3)
    v[1][1][1].b(0)
    ring_step(0, 0, 1)
    v[1][1][0].a2()
    v[0][1][1].end()
    terms(0, 1, False)
    v[1][0][1].b(3)
    v[1][1][0].b(2)
    v[1][1][1].b(2)
    terms(0, 1, True)
    v[1][1][1].b(1)
    v[1][1][1].a2()
    v[1][0][0].end()
    v[1][1][0].b(1)
    ring_step(0, 0, 2)
    v[1][1][0].b(3)
    ring_step(0, 1, 0)
    v[1][0][1].end()
    terms(1, 0, False)
    v[1][1][1].b(3)
    terms(1, 0, True)
    v[1][1][0].end()
    ring_step(0, 0, 3)
    ring_step(1, 0, 0)
    v[1][1][1].end()
    terms(1, 1, False)
    ring_step(0, 1, 1)
    terms(1, 1, True)
    ring_end(0, 0)
    ring_step(1, 1, 0)
    ring_step(1, 0, 1)
    ring_step(0, 1, 2)
    ring_step(1, 1, 1)
    ring_step(1, 0, 2)
    ring_step(0, 1, 3)
    ring_step(1, 1, 2)
    ring_step(1, 0, 3)
    ring_end(0, 1)
    hand_over(0)
    ring_step(1, 1, 3)
    ring_end(1, 0)
    ring_end(1, 1)
    hand_over(1)
    finish(0)
    finish(1)
    for copy in sent:
        copy.wait_send()
    assert len(ids) <= N_SEMS, len(ids)


def local(tokens, norm_gain, gate_weight, linear_weight, output_weight):
    vmem = pl.BlockSpec(memory_space=pltpu.VMEM)
    return pl.pallas_call(
        kernel,
        out_shape=jax.ShapeDtypeStruct((4 * TB, DB), BF),
        in_specs=[vmem] * 5,
        out_specs=vmem,
        scratch_shapes=[
            pltpu.VMEM((2, 4 * FB, DB), BF),
            pltpu.VMEM((4, 4, 2, 4, FB, DB), BF),
            pltpu.VMEM((2, 4, 4, 4, FB, HB), BF),
            pltpu.VMEM((4, TB + GR, DB), BF),
            pltpu.VMEM((2, 2, 4, 4, TB + GR, DB), BF),
            pltpu.VMEM((16, 4 * TB, DB), BF),
            pltpu.VMEM((2, 4 * TB, 4 * FB), F32),
            pltpu.VMEM((4 * TB, 4 * FB), BF),
            pltpu.VMEM((2, 2, 2, 4 * TB, DB), F32),
            pltpu.VMEM((2, 2, 2, 4 * TB, DB), BF),
            pltpu.VMEM((2, 2, 2, 4 * TB, DB), BF),
            pltpu.VMEM((2, 2, 2, 4, TB, DB), BF),
            pltpu.VMEM((2, 2, 2, 4, TB, DB), BF),
            pltpu.VMEM((2, 4, TB, HB), BF),
            pltpu.VMEM((2, 4, TB, HB), BF),
            pltpu.SemaphoreType.DMA((N_SEMS,)),
            pltpu.SemaphoreType.DMA((N_SEMS,)),
        ],
        compiler_params=pltpu.CompilerParams(
            collective_id=0, has_side_effects=True, vmem_limit_bytes=60 * 1024 * 1024
        ),
    )(tokens, norm_gain.reshape(1, DB), gate_weight, linear_weight, output_weight)


def solution(mesh):
    return jax.shard_map(
        local,
        mesh=mesh,
        in_specs=(P("row", "col"), P("col"), P("row", "col"), P("row", "col"), P("col", "row")),
        out_specs=P("row", "col"),
        check_vma=False,
    )
```

```python
import jax
import jax.numpy as jnp
from jax import lax
from jax.experimental import pallas as pl
from jax.experimental.pallas import tpu as pltpu
from jax.sharding import PartitionSpec as P

MESH = pl.DeviceIdType.MESH
BF, F32 = jnp.bfloat16, jnp.float32
FB = 160
DB = 256
HB = DB // 2
TB = 128
GR = 16
N_SEND, N_RECV = 15, 190
NT = (((1,), (1,)), ((), ()))

G_WAYS = ((("x", -1), ("y", 1)), (("x", 1), ("y", -1)), (("x", -1), ("y", 1)), (("x", 1), ("y", -1)))
V_WAYS = (((("x", 1), ("y", 1)), (("x", -1), ("y", -1))), ((("x", -1), ("y", 1)), (("x", 1), ("x", -1))))


def wrap(v, n):
    return lax.rem(v + n, n)


def kernel(
    tok, gain, gw, lw, ow, out,
    wt, gl, w2, tst, tks, nrm, acc, hid, part, stx, srx, rtx, rrx, own_tx, land, send, recv,
):
    row, col = lax.axis_index("row"), lax.axis_index("col")
    zh, y = lax.div(row, 4), lax.rem(row, 4)
    zl, x, k = lax.div(col, 8), lax.rem(lax.div(col, 2), 4), lax.rem(col, 2)
    z = zh * 2 + zl

    def device(dz=0, dy=0, dx=0, dk=0):
        nz, ny, nx = wrap(z + dz, 8), wrap(y + dy, 4), wrap(x + dx, 4)
        return (lax.div(nz, 2) * 4 + ny, lax.rem(nz, 2) * 8 + nx * 2 + lax.rem(k + dk, 2))

    def owner(dz, nx):
        nz = wrap(z + dz, 8)
        return (lax.div(nz, 2) * 4 + y, lax.rem(nz, 2) * 8 + nx * 2 + k)

    peers = (
        [device(dz=d) for d in (1, -1, 2, -2, 4)]
        + [device(dx=d) for d in (1, -1, 2)]
        + [device(dz=d, dx=e) for d in (1, -1) for e in (1, -1, 2)]
        + [device(dy=d) for d in (1, -1)]
        + [device(dk=1)]
    )
    barrier = pltpu.get_barrier_semaphore()
    for peer in peers:
        pl.semaphore_signal(barrier, inc=1, device_id=peer, device_id_type=MESH)

    wt[0] = gw[...].T
    wt[1] = lw[...].T
    pl.semaphore_wait(barrier, len(peers))

    ids, kinds = {}, {}

    def copy_of(name, kind, src, dst, to):
        i = ids.setdefault(name, len(ids))
        o = kinds.setdefault(kind, len(kinds))
        return pltpu.make_async_remote_copy(
            src_ref=src, dst_ref=dst, send_sem=send.at[o], recv_sem=recv.at[i],
            device_id=to, device_id_type=MESH,
        )

    def push(name, kind, src, dst, to):
        copy_of(name, kind, src, dst, to).start()

    def arrive(name, dst):
        copy_of(name, "gz", dst, dst, device(dk=1)).wait_recv()

    def sent(kind, src):
        copy_of(("ta",), kind, src, src, device(dk=1)).wait_send()

    def token_block(dz):
        nz = wrap(z + dz, 8)
        return tks.at[lax.rem(nz, 2), k, lax.div(nz, 2)]

    def rows_for(d):
        return pl.ds(pl.multiple_of(wrap(zh + d, 4) * FB, 16), FB)

    def exchange_inputs(e):
        push(("gz", 4 - e), "gz", wt.at[:, rows_for(e), :], gl.at[zh, y, :, x], device(dz=2 * e))

    def exchange_outputs():
        for c in range(2):
            for e in (1, 3, 2):
                half = pl.ds(c * HB, HB)
                push(("wz", c), "wz", ow.at[rows_for(e), half], w2.at[c, zh, y, x], device(dz=2 * e))

    class Unit:
        def __init__(self, kind, u, tag, first, way):
            self.kind, self.u, self.first, self.way = kind, u, first, way
            self.tag = (kind, tag)
            self.p, self.q = (x, y) if first == "x" else (y, x)

        def block(self, df, ds):
            f, s = wrap(self.p + df, 4), wrap(self.q + ds, 4)
            yy, xx = (s, f) if self.first == "x" else (f, s)
            if self.kind < 2:
                return gl.at[self.u, yy, self.kind, xx]
            return w2.at[self.kind - 2, self.u, yy, xx]

        def along(self, step, second=False):
            return device(dx=step) if (self.first == "x") != second else device(dy=step)

        def go(self, name, j, df, ds, step, second=False):
            ref = self.block(df, ds)
            last = name == "O" or (name, j) in (("R", 0), ("L", 1), ("L", 2), ("R", 3))
            size = "g" if self.kind < 2 else "w"
            key = (self.tag, "end") if last else (self.tag, name, j)
            push(key, (size, second), ref, ref, self.along(step, second))

        def get(self, name, j, df, ds):
            arrive((self.tag, name, j), self.block(df, ds))

        def spread(self, j):
            df = (0, -1, 1, 2)[j]
            self.go("L", j, df, 0, 1, True)
            self.go("R", j, df, 0, -1, True)

        def a0(self):
            self.go("l", 0, 0, 0, 1)
            self.go("r", 0, 0, 0, -1)
            self.spread(0)

        def a1l(self):
            self.get("l", 0, -1, 0)
            if self.way > 0:
                self.go("o", 0, -1, 0, 1)
            self.spread(1)

        def a1r(self):
            self.get("r", 0, 1, 0)
            if self.way < 0:
                self.go("o", 0, 1, 0, -1)
            self.spread(2)

        def a2(self):
            self.get("o", 0, 2, 0)
            self.spread(3)

        def b(self, j):
            df = (0, -1, 1, 2)[j]
            if j in (0, 3):
                self.get("L", j, df, -1)
                self.go("O", j, df, -1, 1, True)
            else:
                self.get("R", j, df, 1)
                self.go("O", j, df, 1, -1, True)

        def end(self):
            eight = gl.at[0, 0:2, 0] if self.kind < 2 else w2.at[0, 0, 0:2]
            arrive((self.tag, "end"), eight)

    def unit_of(d):
        return wrap(zh + d, 4)

    def pair(n, d):
        return [Unit(i, unit_of(d), d, *G_WAYS[n][i]) for i in range(2)]

    g = [pair(n, d) for n, d in enumerate((0, 1, 3, 2))]
    v = [
        [
            [Unit(2 + c, u, u, *V_WAYS[c][h][i]) for i, u in enumerate((h, 2 + h))]
            for h in range(2)
        ]
        for c in range(2)
    ]

    def begin():
        gl[zh, y, :, x] = wt[:, rows_for(0), :]
        g[0][0].a0()
        g[0][1].a0()
        exchange_inputs(1)
        exchange_inputs(3)
        for i in range(4):
            tst[i, 0:TB] = tok[i * TB : (i + 1) * TB]
            tst[i, TB : TB + GR] = jnp.broadcast_to(gain[...], (GR, DB))
        for e in (1, 3, 2):
            push(("ta",), "ta", tst.at[wrap(x + e, 4)], tks.at[zl, k, zh, x], device(dx=e))
        tks[zl, k, zh, x] = tst[x]
        for c in range(2):
            w2[c, zh, y, x] = ow[rows_for(0), c * HB : (c + 1) * HB]
        acc[...] = jnp.zeros_like(acc)

    def weights_in(d):
        arrive(("gz", d), gl.at[unit_of(d), y, :, x])

    def outputs_in(c):
        arrive(("wz", c), w2.at[c, 0, 0, 0:3])

    def tokens_first():
        arrive(("ta",), tks.at[0, 0, 0, 0:3])
        own = token_block(0)
        push(("tm", 1), "tm", own, own, device(dz=-1))
        push(("tp", 1), "tp", own, own, device(dz=1))
        push(("s",), "s", own, own, device(dk=1))
        exchange_inputs(2)

    def tokens_down(m):
        block = token_block(m)
        arrive(("tm", m), block)
        if m < 4:
            push(("tm", m + 1), "tm", block, block, device(dz=-1))
        push(("s",), "s", block, block, device(dk=1))

    def tokens_up(m):
        block = token_block(-m)
        arrive(("tp", m), block)
        if m < 3:
            push(("tp", m + 1), "tp", block, block, device(dz=1))
        push(("s",), "s", block, block, device(dk=1))
        if m == 2:
            exchange_outputs()

    def tokens_last():
        arrive(("s",), tks.at[:, 0])

    def normalise(h):
        spots = [(a, b, c) for a in range(2) for b in range(2) for c in range(4)]

        total = jnp.zeros((TB, DB), F32)
        for a, b, c in spots:
            v = tks[a, b, h, c, 0:TB, :].astype(F32)
            total = total + v * v
        mean = jnp.sum(total, axis=1, keepdims=True) * (1.0 / 4096.0)
        scale = lax.rsqrt(mean + 1e-06)
        for a, b, c in spots:
            v = tks[a, b, h, c, 0:TB, :].astype(F32)
            g = tks[a, b, h, c, TB : TB + GR, :].astype(F32)[0:1, :]
            nrm[a * 8 + c * 2 + b, h * TB : (h + 1) * TB, :] = (v * scale * g).astype(BF)

    def project(n, t):
        u = g[n][0].u
        for a in range(2):
            right = gl[u, t, a].reshape(4 * FB, DB)
            acc[a] += lax.dot_general(nrm[u * 4 + t], right, NT, preferred_element_type=F32)

    def activate(q):
        @pl.loop(2 * q, 2 * q + 2)
        def _(t):
            rows = pl.ds(pl.multiple_of(t * 64, 64), 64)
            hid[rows, :] = (jax.nn.gelu(acc[0, rows, :], approximate=True) * acc[1, rows, :]).astype(BF)

    def terms(c, h, mine):
        core = k if mine else 1 - k
        for a in range(2):
            blocks = [w2[c, 2 * a + h, 2 * i + core].reshape(4 * FB, HB) for i in range(2)]
            right = jnp.concatenate(blocks, axis=1)
            term = jnp.dot(hid[...], right, preferred_element_type=F32)
            if mine:
                part[c, h, a] = term
            else:
                stx[c, h, a] = term.astype(BF)
                push(("c", c, h), "c", stx.at[c, h, a], srx.at[c, h, a], device(dk=1))

    def ring_value(c, h, i, dz):
        nz = wrap(z + dz, 8)
        a, rows = lax.rem(nz, 2), pl.ds(pl.multiple_of(lax.div(nz, 2) * TB, TB), TB)
        lanes = pl.ds(i * HB, HB)
        return part[c, h, a, rows, lanes] + srx[c, h, a, rows, lanes].astype(F32)

    def own_share(c, h):
        for i in range(2):
            nx = 2 * h + i
            own_tx[c, nx] = ring_value(c, h, i, 0).astype(BF)

            @pl.when(x != nx)
            def _():
                push(("fo", c), "fo", own_tx.at[c, nx], land.at[c, 2, x], owner(0, nx))

            @pl.when(x == nx)
            def _():
                land[c, 2, nx] = own_tx[c, nx]

    def ring_step(c, h, i, s):
        if s == 0 and i == 0:
            arrive(("c", c, h), srx.at[c, h])
        for way in (0, 1):
            length = 4 if h == way else 3
            if s >= length:
                continue
            sign = 1 if way == 0 else -1
            value = ring_value(c, h, i, sign * (length - s))
            if s > 0:
                arrive(("r", c, h, i, way, s - 1), rrx.at[c, h, i, way, s - 1])
                value = value + rrx[c, h, i, way, s - 1].astype(F32)
            rtx[c, h, i, way, s] = value.astype(BF)
            src = rtx.at[c, h, i, way, s]
            if s < length - 1:
                push(("r", c, h, i, way, s), ("r", length), src, rrx.at[c, h, i, way, s], device(dz=sign))
            else:
                push(("fr", c), "fr", src, land.at[c, way, x], owner(sign, 2 * h + i))

    def finish(c):
        arrive(("fr", c), land.at[c, 0:2])
        arrive(("fo", c), land.at[c, 2, 0:3])
        for nx in range(4):
            total = land[c, 0, nx].astype(F32) + land[c, 1, nx].astype(F32)
            total = total + land[c, 2, nx].astype(F32)
            out[nx * TB : (nx + 1) * TB, c * HB : (c + 1) * HB] = total.astype(BF)

    begin()
    g[0][0].a1l()
    g[0][0].a1r()
    g[0][0].b(0)
    g[0][1].b(0)
    g[0][1].a1l()
    g[0][1].a1r()
    g[0][0].b(1)
    g[0][0].a2()
    g[0][0].b(2)
    weights_in(3)
    weights_in(1)
    g[1][0].a0()
    g[0][1].b(1)
    tokens_first()
    g[0][1].b(2)
    g[0][1].a2()
    g[1][1].a0()
    g[1][0].a1r()
    g[0][0].b(3)
    g[1][0].b(0)
    g[1][0].a1l()
    g[1][1].a1l()
    g[1][1].a1r()
    g[0][1].b(3)
    g[1][0].b(2)
    g[1][1].b(0)
    tokens_down(1)
    tokens_up(1)
    g[0][0].end()
    g[1][0].b(1)
    g[2][0].a0()
    g[1][0].a2()
    g[1][1].b(1)
    g[1][1].a2()
    g[1][1].b(2)
    g[2][1].a0()
    g[2][0].a1r()
    g[2][0].b(0)
    g[0][1].end()
    g[1][0].b(3)
    g[2][1].a1l()
    tokens_down(2)
    g[2][0].a1l()
    g[2][1].a1r()
    g[1][1].b(3)
    g[2][0].b(2)
    g[2][1].b(0)
    g[2][0].a2()
    weights_in(2)
    g[1][0].end()
    g[2][0].b(1)
    g[3][0].a0()
    g[2][1].b(1)
    g[2][1].a2()
    g[2][1].b(2)
    g[3][1].a0()
    g[1][1].end()
    g[3][0].a1r()
    g[2][0].b(3)
    tokens_down(3)
    tokens_up(2)
    g[3][0].b(0)
    g[3][0].a1l()
    g[3][1].a1l()
    g[3][1].a1r()
    g[2][1].b(3)
    g[3][0].b(2)
    g[3][1].b(0)
    g[2][0].end()
    g[3][0].b(1)
    g[3][0].a2()
    g[3][1].b(1)
    g[3][1].a2()
    g[3][1].b(2)
    tokens_down(4)
    tokens_up(3)
    g[3][0].b(3)
    g[2][1].end()
    tokens_last()
    normalise(0)
    normalise(1)
    normalise(2)
    outputs_in(0)
    g[3][1].b(3)
    v[0][0][0].a0()
    v[0][0][1].a0()
    normalise(3)
    v[0][1][0].a0()
    project(0, 0)
    v[0][1][1].a0()
    project(0, 1)
    project(0, 2)
    v[0][0][0].a1r()
    v[0][0][0].b(0)
    project(0, 3)
    v[0][0][1].a1l()
    v[0][0][1].a1r()
    project(1, 0)
    outputs_in(1)
    v[0][0][0].a1l()
    v[0][1][0].a1r()
    v[0][1][0].b(0)
    project(1, 1)
    v[0][0][1].b(0)
    v[0][1][1].a1l()
    v[0][1][1].a1r()
    project(1, 2)
    v[0][0][0].b(2)
    v[0][1][0].a1l()
    project(1, 3)
    v[0][0][1].b(1)
    v[0][1][1].b(0)
    project(2, 0)
    v[0][0][0].b(1)
    v[0][0][1].b(2)
    project(2, 1)
    v[0][0][1].a2()
    v[0][1][0].a2()
    v[0][1][0].b(2)
    project(2, 2)
    v[0][1][1].b(1)
    v[0][1][1].a2()
    project(2, 3)
    v[0][0][0].a2()
    g[3][0].end()
    v[0][1][1].b(2)
    g[3][1].end()
    v[1][0][0].a0()
    project(3, 0)
    v[0][1][0].b(1)
    v[1][0][1].a0()
    project(3, 1)
    project(3, 2)
    v[0][1][0].b(3)
    project(3, 3)
    v[1][1][0].a0()
    v[0][0][0].b(3)
    activate(0)
    activate(1)
    v[0][0][1].b(3)
    v[1][0][0].b(0)
    activate(2)
    v[0][1][1].b(3)
    v[1][0][1].a1l()
    v[1][1][1].a0()
    activate(3)
    v[1][0][0].a1l()
    v[1][0][0].a1r()
    v[0][1][0].end()
    v[1][0][1].b(0)
    v[1][1][0].b(0)
    v[1][0][1].a1r()
    v[1][1][0].a1l()
    v[0][0][0].end()
    v[1][1][0].a1r()
    v[0][0][1].end()
    terms(0, 0, False)
    v[1][0][1].b(1)
    v[1][0][1].a2()
    terms(0, 0, True)
    v[1][0][0].b(1)
    v[1][1][1].a1r()
    v[1][1][1].b(0)
    v[0][1][1].end()
    v[1][0][0].a2()
    v[1][0][0].b(2)
    terms(0, 1, False)
    v[1][0][1].b(2)
    v[1][1][0].b(1)
    v[1][1][1].a1l()
    terms(0, 1, True)
    ring_step(0, 0, 0, 0)
    ring_step(0, 0, 1, 0)
    v[1][1][0].b(2)
    own_share(0, 0)
    v[1][1][0].a2()
    v[1][1][1].a2()
    v[1][1][1].b(2)
    ring_step(0, 1, 0, 0)
    ring_step(0, 1, 1, 0)
    v[1][0][1].b(3)
    own_share(0, 1)
    ring_step(0, 0, 0, 1)
    ring_step(0, 0, 1, 1)
    v[1][0][0].b(3)
    v[1][1][1].b(1)
    v[1][0][1].end()
    ring_step(0, 1, 0, 1)
    v[1][1][0].b(3)
    ring_step(0, 1, 1, 1)
    v[1][1][1].b(3)
    ring_step(0, 0, 0, 2)
    v[1][0][0].end()
    terms(1, 0, False)
    ring_step(0, 0, 1, 2)
    terms(1, 0, True)
    v[1][1][0].end()
    ring_step(0, 1, 0, 2)
    v[1][1][1].end()
    terms(1, 1, False)
    ring_step(0, 1, 1, 2)
    terms(1, 1, True)
    ring_step(1, 0, 0, 0)
    ring_step(1, 0, 1, 0)
    ring_step(0, 0, 0, 3)
    own_share(1, 0)
    ring_step(0, 0, 1, 3)
    ring_step(1, 1, 0, 0)
    ring_step(1, 1, 1, 0)
    own_share(1, 1)
    ring_step(0, 1, 0, 3)
    ring_step(1, 0, 0, 1)
    ring_step(0, 1, 1, 3)
    ring_step(1, 0, 1, 1)
    ring_step(1, 1, 0, 1)
    ring_step(1, 1, 1, 1)
    ring_step(1, 0, 0, 2)
    ring_step(1, 0, 1, 2)
    ring_step(1, 1, 0, 2)
    ring_step(1, 1, 1, 2)
    ring_step(1, 0, 0, 3)
    ring_step(1, 0, 1, 3)
    ring_step(1, 1, 0, 3)
    ring_step(1, 1, 1, 3)
    finish(0)
    finish(1)
    for kind, src in (
        ("ta", tks.at[0, 0, 0, 0:3]),
        ("gz", gl.at[0, 0:3, :, 0]),
        ("wz", w2.at[:, 0, 0, 0:3]),
        (("g", True), gl.at[:, 0:3]),
        (("g", False), gl.at[:, 0:3, :, 0]),
        (("w", True), w2.at[:, :, 0:3]),
        (("w", False), w2.at[:, :, 0:3, 0]),
        ("tm", tks.at[0, 0]),
        ("tp", tks.at[0, 0, 0:3]),
        ("s", tks.at[0]),
        ("c", stx),
        (("r", 4), rtx.at[:, :, :, 0, 0:3]),
        (("r", 3), rtx.at[:, :, :, 0, 0:2]),
        ("fr", rtx.at[:, :, :, :, 0]),
        ("fo", own_tx.at[:, 0:3]),
    ):
        sent(kind, src)
    assert len(ids) == N_RECV and len(kinds) == N_SEND, (len(ids), len(kinds))


def local(tokens, norm_gain, gate_weight, linear_weight, output_weight):
    vmem = pl.BlockSpec(memory_space=pltpu.VMEM)
    return pl.pallas_call(
        kernel,
        out_shape=jax.ShapeDtypeStruct((4 * TB, DB), BF),
        in_specs=[vmem] * 5,
        out_specs=vmem,
        scratch_shapes=[
            pltpu.VMEM((2, 4 * FB, DB), BF),
            pltpu.VMEM((4, 4, 2, 4, FB, DB), BF),
            pltpu.VMEM((2, 4, 4, 4, FB, HB), BF),
            pltpu.VMEM((4, TB + GR, DB), BF),
            pltpu.VMEM((2, 2, 4, 4, TB + GR, DB), BF),
            pltpu.VMEM((16, 4 * TB, DB), BF),
            pltpu.VMEM((2, 4 * TB, 4 * FB), F32),
            pltpu.VMEM((4 * TB, 4 * FB), BF),
            pltpu.VMEM((2, 2, 2, 4 * TB, DB), F32),
            pltpu.VMEM((2, 2, 2, 4 * TB, DB), BF),
            pltpu.VMEM((2, 2, 2, 4 * TB, DB), BF),
            pltpu.VMEM((2, 2, 2, 2, 4, TB, HB), BF),
            pltpu.VMEM((2, 2, 2, 2, 3, TB, HB), BF),
            pltpu.VMEM((2, 4, TB, HB), BF),
            pltpu.VMEM((2, 3, 4, TB, HB), BF),
            pltpu.SemaphoreType.DMA((N_SEND,)),
            pltpu.SemaphoreType.DMA((N_RECV,)),
        ],
        compiler_params=pltpu.CompilerParams(
            collective_id=0, has_side_effects=True, vmem_limit_bytes=60 * 1024 * 1024
        ),
    )(tokens, norm_gain.reshape(1, DB), gate_weight, linear_weight, output_weight)


def solution(mesh):
    return jax.shard_map(
        local,
        mesh=mesh,
        in_specs=(P("row", "col"), P("col"), P("row", "col"), P("row", "col"), P("col", "row")),
        out_specs=P("row", "col"),
        check_vma=False,
    )
```

```python
import jax
import jax.numpy as jnp
from jax import lax
from jax.experimental import pallas as pl
from jax.experimental.pallas import tpu as pltpu
from jax.sharding import PartitionSpec as P

MESH = pl.DeviceIdType.MESH
BF, F32 = jnp.bfloat16, jnp.float32
FB = 160
DB = 256
HB = DB // 2
TB = 128
GR = 16
N_SEND, N_RECV = 15, 190
NT = (((1,), (1,)), ((), ()))

G_WAYS = ((("x", -1), ("y", 1)), (("x", 1), ("y", -1)), (("x", -1), ("y", 1)), (("x", 1), ("y", -1)))
V_WAYS = (((("x", -1), ("y", 1)), (("x", -1), ("y", -1))), ((("x", -1), ("y", 1)), (("x", 1), ("x", -1))))


def wrap(v, n):
    return lax.rem(v + n, n)


def kernel(
    tok, gain, gw, lw, ow, out,
    wt, gl, w2, tst, tks, nrm, acc, hid, part, stx, srx, rtx, rrx, own_tx, land, send, recv,
):
    row, col = lax.axis_index("row"), lax.axis_index("col")
    zh, y = lax.div(row, 4), lax.rem(row, 4)
    zl, x, k = lax.div(col, 8), lax.rem(lax.div(col, 2), 4), lax.rem(col, 2)
    z = zh * 2 + zl

    def device(dz=0, dy=0, dx=0, dk=0):
        nz, ny, nx = wrap(z + dz, 8), wrap(y + dy, 4), wrap(x + dx, 4)
        return (lax.div(nz, 2) * 4 + ny, lax.rem(nz, 2) * 8 + nx * 2 + lax.rem(k + dk, 2))

    def owner(dz, nx):
        nz = wrap(z + dz, 8)
        return (lax.div(nz, 2) * 4 + y, lax.rem(nz, 2) * 8 + nx * 2 + k)

    peers = (
        [device(dz=d) for d in (1, -1, 2, -2, 4)]
        + [device(dx=d) for d in (1, -1, 2)]
        + [device(dz=d, dx=e) for d in (1, -1) for e in (1, -1, 2)]
        + [device(dy=d) for d in (1, -1)]
        + [device(dk=1)]
    )
    barrier = pltpu.get_barrier_semaphore()
    for peer in peers:
        pl.semaphore_signal(barrier, inc=1, device_id=peer, device_id_type=MESH)

    wt[0] = gw[...].T
    wt[1] = lw[...].T
    pl.semaphore_wait(barrier, len(peers))

    ids, kinds = {}, {}

    def copy_of(name, kind, src, dst, to):
        i = ids.setdefault(name, len(ids))
        o = kinds.setdefault(kind, len(kinds))
        return pltpu.make_async_remote_copy(
            src_ref=src, dst_ref=dst, send_sem=send.at[o], recv_sem=recv.at[i],
            device_id=to, device_id_type=MESH,
        )

    def push(name, kind, src, dst, to):
        copy_of(name, kind, src, dst, to).start()

    def arrive(name, dst):
        copy_of(name, "gz", dst, dst, device(dk=1)).wait_recv()

    def sent(kind, src):
        copy_of(("ta",), kind, src, src, device(dk=1)).wait_send()

    def token_block(dz):
        nz = wrap(z + dz, 8)
        return tks.at[lax.rem(nz, 2), k, lax.div(nz, 2)]

    def rows_for(d):
        return pl.ds(pl.multiple_of(wrap(zh + d, 4) * FB, 16), FB)

    def exchange_inputs(e):
        push(("gz", 4 - e), "gz", wt.at[:, rows_for(e), :], gl.at[zh, y, :, x], device(dz=2 * e))

    def exchange_outputs():
        for c in range(2):
            for e in (1, 3, 2):
                half = pl.ds(c * HB, HB)
                push(("wz", c), "wz", ow.at[rows_for(e), half], w2.at[c, zh, y, x], device(dz=2 * e))

    class Unit:
        def __init__(self, kind, u, tag, first, way):
            self.kind, self.u, self.first, self.way = kind, u, first, way
            self.tag = (kind, tag)
            self.p, self.q = (x, y) if first == "x" else (y, x)

        def block(self, df, ds):
            f, s = wrap(self.p + df, 4), wrap(self.q + ds, 4)
            yy, xx = (s, f) if self.first == "x" else (f, s)
            if self.kind < 2:
                return gl.at[self.u, yy, self.kind, xx]
            return w2.at[self.kind - 2, self.u, yy, xx]

        def along(self, step, second=False):
            return device(dx=step) if (self.first == "x") != second else device(dy=step)

        def go(self, name, j, df, ds, step, second=False):
            ref = self.block(df, ds)
            last = name == "O" or (name, j) in (("R", 0), ("L", 1), ("L", 2), ("R", 3))
            size = "g" if self.kind < 2 else "w"
            key = (self.tag, "end") if last else (self.tag, name, j)
            push(key, (size, second), ref, ref, self.along(step, second))

        def get(self, name, j, df, ds):
            arrive((self.tag, name, j), self.block(df, ds))

        def spread(self, j):
            df = (0, -1, 1, 2)[j]
            self.go("L", j, df, 0, 1, True)
            self.go("R", j, df, 0, -1, True)

        def a0(self):
            self.go("l", 0, 0, 0, 1)
            self.go("r", 0, 0, 0, -1)
            self.spread(0)

        def a1l(self):
            self.get("l", 0, -1, 0)
            if self.way > 0:
                self.go("o", 0, -1, 0, 1)
            self.spread(1)

        def a1r(self):
            self.get("r", 0, 1, 0)
            if self.way < 0:
                self.go("o", 0, 1, 0, -1)
            self.spread(2)

        def a2(self):
            self.get("o", 0, 2, 0)
            self.spread(3)

        def b(self, j):
            df = (0, -1, 1, 2)[j]
            if j in (0, 3):
                self.get("L", j, df, -1)
                self.go("O", j, df, -1, 1, True)
            else:
                self.get("R", j, df, 1)
                self.go("O", j, df, 1, -1, True)

        def end(self):
            eight = gl.at[0, 0:2, 0] if self.kind < 2 else w2.at[0, 0, 0:2]
            arrive((self.tag, "end"), eight)

    def unit_of(d):
        return wrap(zh + d, 4)

    def pair(n, d):
        return [Unit(i, unit_of(d), d, *G_WAYS[n][i]) for i in range(2)]

    g = [pair(n, d) for n, d in enumerate((0, 1, 3, 2))]
    v = [
        [
            [Unit(2 + c, u, u, *V_WAYS[c][h][i]) for i, u in enumerate((h, 2 + h))]
            for h in range(2)
        ]
        for c in range(2)
    ]

    def begin():
        gl[zh, y, :, x] = wt[:, rows_for(0), :]
        g[0][0].a0()
        g[0][1].a0()
        exchange_inputs(1)
        exchange_inputs(3)
        for i in range(4):
            tst[i, 0:TB] = tok[i * TB : (i + 1) * TB]
            tst[i, TB : TB + GR] = jnp.broadcast_to(gain[...], (GR, DB))
        for e in (1, 3, 2):
            push(("ta",), "ta", tst.at[wrap(x + e, 4)], tks.at[zl, k, zh, x], device(dx=e))
        tks[zl, k, zh, x] = tst[x]
        for c in range(2):
            w2[c, zh, y, x] = ow[rows_for(0), c * HB : (c + 1) * HB]
        acc[...] = jnp.zeros_like(acc)

    def weights_in(d):
        arrive(("gz", d), gl.at[unit_of(d), y, :, x])

    def outputs_in(c):
        arrive(("wz", c), w2.at[c, 0, 0, 0:3])

    def tokens_first():
        arrive(("ta",), tks.at[0, 0, 0, 0:3])
        own = token_block(0)
        push(("tm", 1), "tm", own, own, device(dz=-1))
        push(("tp", 1), "tp", own, own, device(dz=1))
        push(("s",), "s", own, own, device(dk=1))
        exchange_inputs(2)

    def tokens_down(m):
        block = token_block(m)
        arrive(("tm", m), block)
        if m < 4:
            push(("tm", m + 1), "tm", block, block, device(dz=-1))
        push(("s",), "s", block, block, device(dk=1))

    def tokens_up(m):
        block = token_block(-m)
        arrive(("tp", m), block)
        if m < 3:
            push(("tp", m + 1), "tp", block, block, device(dz=1))
        push(("s",), "s", block, block, device(dk=1))
        if m == 2:
            exchange_outputs()

    def tokens_last():
        arrive(("s",), tks.at[:, 0])

    def normalise():
        spots = [(a, b, c) for a in range(2) for b in range(2) for c in range(4)]

        @pl.loop(0, 4)
        def _(h):
            total = jnp.zeros((TB, DB), F32)
            for a, b, c in spots:
                v = tks[a, b, h, c, 0:TB, :].astype(F32)
                total = total + v * v
            mean = jnp.sum(total, axis=1, keepdims=True) * (1.0 / 4096.0)
            scale = lax.rsqrt(mean + 1e-06)
            rows = pl.ds(pl.multiple_of(h * TB, TB), TB)
            for a, b, c in spots:
                v = tks[a, b, h, c, 0:TB, :].astype(F32)
                g = tks[a, b, h, c, TB : TB + GR, :].astype(F32)[0:1, :]
                nrm[a * 8 + c * 2 + b, rows, :] = (v * scale * g).astype(BF)

    def project(n, t):
        u = g[n][0].u
        for a in range(2):
            right = gl[u, t, a].reshape(4 * FB, DB)
            acc[a] += lax.dot_general(nrm[u * 4 + t], right, NT, preferred_element_type=F32)

    def activate(q):
        @pl.loop(2 * q, 2 * q + 2)
        def _(t):
            rows = pl.ds(pl.multiple_of(t * 64, 64), 64)
            hid[rows, :] = (jax.nn.gelu(acc[0, rows, :], approximate=True) * acc[1, rows, :]).astype(BF)

    def terms(c, h, mine):
        core = k if mine else 1 - k
        for a in range(2):
            blocks = [w2[c, 2 * a + h, 2 * i + core].reshape(4 * FB, HB) for i in range(2)]
            right = jnp.concatenate(blocks, axis=1)
            term = jnp.dot(hid[...], right, preferred_element_type=F32)
            if mine:
                part[c, h, a] = term
            else:
                stx[c, h, a] = term.astype(BF)
                push(("c", c, h), "c", stx.at[c, h, a], srx.at[c, h, a], device(dk=1))

    def ring_value(c, h, i, dz):
        nz = wrap(z + dz, 8)
        a, rows = lax.rem(nz, 2), pl.ds(pl.multiple_of(lax.div(nz, 2) * TB, TB), TB)
        lanes = pl.ds(i * HB, HB)
        return part[c, h, a, rows, lanes] + srx[c, h, a, rows, lanes].astype(F32)

    def own_share(c, h):
        for i in range(2):
            nx = 2 * h + i
            own_tx[c, nx] = ring_value(c, h, i, 0).astype(BF)

            @pl.when(x != nx)
            def _():
                push(("fo", c), "fo", own_tx.at[c, nx], land.at[c, 2, x], owner(0, nx))

            @pl.when(x == nx)
            def _():
                land[c, 2, nx] = own_tx[c, nx]

    def ring_step(c, h, i, s):
        if s == 0 and i == 0:
            arrive(("c", c, h), srx.at[c, h])
        for way in (0, 1):
            length = 4 if h == way else 3
            if s >= length:
                continue
            sign = 1 if way == 0 else -1
            value = ring_value(c, h, i, sign * (length - s))
            if s > 0:
                arrive(("r", c, h, i, way, s - 1), rrx.at[c, h, i, way, s - 1])
                value = value + rrx[c, h, i, way, s - 1].astype(F32)
            rtx[c, h, i, way, s] = value.astype(BF)
            src = rtx.at[c, h, i, way, s]
            if s < length - 1:
                push(("r", c, h, i, way, s), ("r", length), src, rrx.at[c, h, i, way, s], device(dz=sign))
            else:
                push(("fr", c), "fr", src, land.at[c, way, x], owner(sign, 2 * h + i))

    def finish(c):
        arrive(("fr", c), land.at[c, 0:2])
        arrive(("fo", c), land.at[c, 2, 0:3])
        for nx in range(4):
            total = land[c, 0, nx].astype(F32) + land[c, 1, nx].astype(F32)
            total = total + land[c, 2, nx].astype(F32)
            out[nx * TB : (nx + 1) * TB, c * HB : (c + 1) * HB] = total.astype(BF)

    begin()
    g[0][0].a1l()
    g[0][0].a1r()
    g[0][0].b(0)
    g[0][1].b(0)
    g[0][1].a1l()
    g[0][1].a1r()
    g[0][0].b(1)
    g[0][0].a2()
    g[0][0].b(2)
    weights_in(3)
    weights_in(1)
    g[1][0].a0()
    g[0][1].b(1)
    tokens_first()
    g[0][1].b(2)
    g[0][1].a2()
    g[1][1].a0()
    g[1][0].a1r()
    g[0][0].b(3)
    g[1][0].b(0)
    g[1][0].a1l()
    g[1][1].a1l()
    g[1][1].a1r()
    g[0][1].b(3)
    g[1][0].b(2)
    g[1][1].b(0)
    tokens_down(1)
    tokens_up(1)
    g[0][0].end()
    g[1][0].b(1)
    g[2][0].a0()
    g[1][0].a2()
    g[1][1].b(1)
    g[1][1].a2()
    g[1][1].b(2)
    g[2][1].a0()
    g[2][0].a1r()
    g[2][0].b(0)
    g[0][1].end()
    g[1][0].b(3)
    g[2][1].a1l()
    tokens_down(2)
    g[2][0].a1l()
    g[2][1].a1r()
    g[1][1].b(3)
    g[2][0].b(2)
    g[2][1].b(0)
    g[2][0].a2()
    weights_in(2)
    g[1][0].end()
    g[2][0].b(1)
    g[3][0].a0()
    g[2][1].b(1)
    g[2][1].a2()
    g[2][1].b(2)
    g[3][1].a0()
    g[1][1].end()
    g[3][0].a1r()
    g[2][0].b(3)
    tokens_down(3)
    tokens_up(2)
    g[3][0].b(0)
    g[3][0].a1l()
    g[3][1].a1l()
    g[3][1].a1r()
    g[2][1].b(3)
    g[3][0].b(2)
    g[3][1].b(0)
    g[2][0].end()
    g[3][0].b(1)
    g[3][0].a2()
    g[3][1].b(1)
    g[3][1].a2()
    g[3][1].b(2)
    tokens_down(4)
    tokens_up(3)
    g[3][0].b(3)
    g[2][1].end()
    tokens_last()
    outputs_in(0)
    g[3][1].b(3)
    v[0][0][0].a0()
    v[0][0][1].a0()
    normalise()
    v[0][1][0].a0()
    project(0, 0)
    v[0][1][1].a0()
    project(0, 1)
    project(0, 2)
    v[0][0][0].a1r()
    v[0][0][0].b(0)
    project(0, 3)
    v[0][0][1].a1l()
    v[0][0][1].a1r()
    project(1, 0)
    outputs_in(1)
    v[0][0][0].a1l()
    v[0][1][0].a1r()
    v[0][1][0].b(0)
    project(1, 1)
    v[0][0][1].b(0)
    v[0][1][1].a1l()
    v[0][1][1].a1r()
    project(1, 2)
    v[0][0][0].a2()
    v[0][0][0].b(2)
    v[0][1][0].a1l()
    project(1, 3)
    v[0][0][1].b(1)
    v[0][1][1].b(0)
    project(2, 0)
    v[0][0][0].b(1)
    project(2, 1)
    v[0][0][1].b(2)
    v[0][0][1].a2()
    v[0][1][0].b(2)
    project(2, 2)
    v[0][1][0].a2()
    v[0][1][1].a2()
    project(2, 3)
    v[0][1][1].b(1)
    g[3][0].end()
    g[3][1].end()
    v[0][1][1].b(2)
    v[1][0][0].a0()
    project(3, 0)
    v[1][0][1].a0()
    v[0][0][0].b(3)
    project(3, 1)
    v[0][1][0].b(1)
    project(3, 2)
    project(3, 3)
    v[0][0][1].b(3)
    v[0][1][0].b(3)
    activate(0)
    v[1][1][0].a0()
    activate(1)
    v[0][1][1].b(3)
    v[1][0][0].b(0)
    activate(2)
    v[1][0][0].a1l()
    v[1][0][1].a1l()
    activate(3)
    v[1][0][1].b(0)
    v[0][0][0].end()
    v[1][1][1].a0()
    v[1][0][1].a1r()
    v[0][0][1].end()
    v[1][0][0].a1r()
    terms(0, 0, False)
    v[1][1][0].a1l()
    v[1][1][0].b(0)
    terms(0, 0, True)
    v[1][1][0].a1r()
    v[0][1][0].end()
    v[1][0][0].b(1)
    v[0][1][1].end()
    terms(0, 1, False)
    v[1][0][1].b(1)
    terms(0, 1, True)
    v[1][0][1].a2()
    v[1][0][0].b(2)
    ring_step(0, 0, 0, 0)
    ring_step(0, 0, 1, 0)
    v[1][0][1].b(2)
    v[1][1][1].a1r()
    v[1][1][1].a1l()
    v[1][1][0].b(1)
    v[1][1][1].b(0)
    own_share(0, 0)
    v[1][0][0].a2()
    v[1][1][0].b(2)
    v[1][1][0].a2()
    ring_step(0, 1, 0, 0)
    ring_step(0, 1, 1, 0)
    own_share(0, 1)
    v[1][0][1].b(3)
    ring_step(0, 0, 0, 1)
    v[1][1][1].b(2)
    v[1][1][1].a2()
    ring_step(0, 0, 1, 1)
    v[1][1][1].b(1)
    ring_step(0, 1, 0, 1)
    v[1][0][1].end()
    ring_step(0, 1, 1, 1)
    v[1][0][0].b(3)
    v[1][1][0].b(3)
    ring_step(0, 0, 0, 2)
    ring_step(0, 0, 1, 2)
    v[1][1][1].b(3)
    v[1][0][0].end()
    ring_step(0, 1, 0, 2)
    terms(1, 0, False)
    ring_step(0, 1, 1, 2)
    terms(1, 0, True)
    v[1][1][0].end()
    ring_step(0, 0, 0, 3)
    v[1][1][1].end()
    terms(1, 1, False)
    ring_step(0, 0, 1, 3)
    terms(1, 1, True)
    ring_step(1, 0, 0, 0)
    ring_step(1, 0, 1, 0)
    ring_step(0, 1, 0, 3)
    own_share(1, 0)
    ring_step(0, 1, 1, 3)
    ring_step(1, 1, 0, 0)
    ring_step(1, 1, 1, 0)
    own_share(1, 1)
    ring_step(1, 0, 0, 1)
    ring_step(1, 0, 1, 1)
    ring_step(1, 1, 0, 1)
    ring_step(1, 1, 1, 1)
    ring_step(1, 0, 0, 2)
    ring_step(1, 0, 1, 2)
    ring_step(1, 1, 0, 2)
    ring_step(1, 1, 1, 2)
    ring_step(1, 0, 0, 3)
    ring_step(1, 0, 1, 3)
    ring_step(1, 1, 0, 3)
    ring_step(1, 1, 1, 3)
    finish(0)
    finish(1)
    for kind, src in (
        ("ta", tks.at[0, 0, 0, 0:3]),
        ("gz", gl.at[0, 0:3, :, 0]),
        ("wz", w2.at[:, 0, 0, 0:3]),
        (("g", True), gl.at[:, 0:3]),
        (("g", False), gl.at[:, 0:3, :, 0]),
        (("w", True), w2.at[:, :, 0:3]),
        (("w", False), w2.at[:, :, 0:3, 0]),
        ("tm", tks.at[0, 0]),
        ("tp", tks.at[0, 0, 0:3]),
        ("s", tks.at[0]),
        ("c", stx),
        (("r", 4), rtx.at[:, :, :, 0, 0:3]),
        (("r", 3), rtx.at[:, :, :, 0, 0:2]),
        ("fr", rtx.at[:, :, :, :, 0]),
        ("fo", own_tx.at[:, 0:3]),
    ):
        sent(kind, src)
    assert len(ids) == N_RECV and len(kinds) == N_SEND, (len(ids), len(kinds))


def local(tokens, norm_gain, gate_weight, linear_weight, output_weight):
    vmem = pl.BlockSpec(memory_space=pltpu.VMEM)
    return pl.pallas_call(
        kernel,
        out_shape=jax.ShapeDtypeStruct((4 * TB, DB), BF),
        in_specs=[vmem] * 5,
        out_specs=vmem,
        scratch_shapes=[
            pltpu.VMEM((2, 4 * FB, DB), BF),
            pltpu.VMEM((4, 4, 2, 4, FB, DB), BF),
            pltpu.VMEM((2, 4, 4, 4, FB, HB), BF),
            pltpu.VMEM((4, TB + GR, DB), BF),
            pltpu.VMEM((2, 2, 4, 4, TB + GR, DB), BF),
            pltpu.VMEM((16, 4 * TB, DB), BF),
            pltpu.VMEM((2, 4 * TB, 4 * FB), F32),
            pltpu.VMEM((4 * TB, 4 * FB), BF),
            pltpu.VMEM((2, 2, 2, 4 * TB, DB), F32),
            pltpu.VMEM((2, 2, 2, 4 * TB, DB), BF),
            pltpu.VMEM((2, 2, 2, 4 * TB, DB), BF),
            pltpu.VMEM((2, 2, 2, 2, 4, TB, HB), BF),
            pltpu.VMEM((2, 2, 2, 2, 3, TB, HB), BF),
            pltpu.VMEM((2, 4, TB, HB), BF),
            pltpu.VMEM((2, 3, 4, TB, HB), BF),
            pltpu.SemaphoreType.DMA((N_SEND,)),
            pltpu.SemaphoreType.DMA((N_RECV,)),
        ],
        compiler_params=pltpu.CompilerParams(
            collective_id=0, has_side_effects=True, vmem_limit_bytes=60 * 1024 * 1024
        ),
    )(tokens, norm_gain.reshape(1, DB), gate_weight, linear_weight, output_weight)


def solution(mesh):
    return jax.shard_map(
        local,
        mesh=mesh,
        in_specs=(P("row", "col"), P("col"), P("row", "col"), P("row", "col"), P("col", "row")),
        out_specs=P("row", "col"),
        check_vma=False,
    )
```

```python
import jax
import jax.numpy as jnp
from jax import lax
from jax.experimental import pallas as pl
from jax.experimental.pallas import tpu as pltpu
from jax.sharding import PartitionSpec as P

MESH = pl.DeviceIdType.MESH
BF, F32 = jnp.bfloat16, jnp.float32
FB = 160
DB = 256
HB = DB // 2
TB = 128
GR = 16
N_SEND, N_RECV = 15, 190
NT = (((1,), (1,)), ((), ()))

G_WAYS = ((("x", -1), ("y", 1)), (("x", 1), ("y", -1)), (("x", -1), ("y", 1)), (("x", 1), ("y", -1)))
V_WAYS = (((("x", -1), ("y", 1)), (("x", -1), ("y", -1))), ((("x", -1), ("y", 1)), (("x", 1), ("x", -1))))


def wrap(v, n):
    return lax.rem(v + n, n)


def kernel(
    tok, gain, gw, lw, ow, out,
    wt, gl, w2, tst, tks, nrm, acc, hid, part, stx, srx, rtx, rrx, own_tx, land, send, recv,
):
    row, col = lax.axis_index("row"), lax.axis_index("col")
    zh, y = lax.div(row, 4), lax.rem(row, 4)
    zl, x, k = lax.div(col, 8), lax.rem(lax.div(col, 2), 4), lax.rem(col, 2)
    z = zh * 2 + zl

    def device(dz=0, dy=0, dx=0, dk=0):
        nz, ny, nx = wrap(z + dz, 8), wrap(y + dy, 4), wrap(x + dx, 4)
        return (lax.div(nz, 2) * 4 + ny, lax.rem(nz, 2) * 8 + nx * 2 + lax.rem(k + dk, 2))

    def owner(dz, nx):
        nz = wrap(z + dz, 8)
        return (lax.div(nz, 2) * 4 + y, lax.rem(nz, 2) * 8 + nx * 2 + k)

    peers = (
        [device(dz=d) for d in (1, -1, 2, -2, 4)]
        + [device(dx=d) for d in (1, -1, 2)]
        + [device(dz=d, dx=e) for d in (1, -1) for e in (1, -1, 2)]
        + [device(dy=d) for d in (1, -1)]
        + [device(dk=1)]
    )
    barrier = pltpu.get_barrier_semaphore()
    for peer in peers:
        pl.semaphore_signal(barrier, inc=1, device_id=peer, device_id_type=MESH)

    wt[0] = gw[...].T
    wt[1] = lw[...].T
    acc[...] = jnp.zeros_like(acc)
    pl.semaphore_wait(barrier, len(peers))

    ids, kinds = {}, {}

    def copy_of(name, kind, src, dst, to):
        i = ids.setdefault(name, len(ids))
        o = kinds.setdefault(kind, len(kinds))
        return pltpu.make_async_remote_copy(
            src_ref=src, dst_ref=dst, send_sem=send.at[o], recv_sem=recv.at[i],
            device_id=to, device_id_type=MESH,
        )

    def push(name, kind, src, dst, to):
        copy_of(name, kind, src, dst, to).start()

    def arrive(name, dst):
        copy_of(name, "gz", dst, dst, device(dk=1)).wait_recv()

    def sent(kind, src):
        copy_of(("ta",), kind, src, src, device(dk=1)).wait_send()

    def token_block(dz):
        nz = wrap(z + dz, 8)
        return tks.at[lax.rem(nz, 2), k, lax.div(nz, 2)]

    def rows_for(d):
        return pl.ds(pl.multiple_of(wrap(zh + d, 4) * FB, 16), FB)

    def exchange_inputs(e):
        push(("gz", 4 - e), "gz", wt.at[:, rows_for(e), :], gl.at[zh, y, :, x], device(dz=2 * e))

    def exchange_outputs():
        for c in range(2):
            for e in (1, 3, 2):
                half = pl.ds(c * HB, HB)
                push(("wz", c), "wz", ow.at[rows_for(e), half], w2.at[c, zh, y, x], device(dz=2 * e))

    class Unit:
        def __init__(self, kind, u, tag, first, way):
            self.kind, self.u, self.first, self.way = kind, u, first, way
            self.tag = (kind, tag)
            self.p, self.q = (x, y) if first == "x" else (y, x)

        def block(self, df, ds):
            f, s = wrap(self.p + df, 4), wrap(self.q + ds, 4)
            yy, xx = (s, f) if self.first == "x" else (f, s)
            if self.kind < 2:
                return gl.at[self.u, yy, self.kind, xx]
            return w2.at[self.kind - 2, self.u, yy, xx]

        def along(self, step, second=False):
            return device(dx=step) if (self.first == "x") != second else device(dy=step)

        def go(self, name, j, df, ds, step, second=False):
            ref = self.block(df, ds)
            last = name == "O" or (name, j) in (("R", 0), ("L", 1), ("L", 2), ("R", 3))
            size = "g" if self.kind < 2 else "w"
            key = (self.tag, "end") if last else (self.tag, name, j)
            push(key, (size, second), ref, ref, self.along(step, second))

        def get(self, name, j, df, ds):
            arrive((self.tag, name, j), self.block(df, ds))

        def spread(self, j):
            df = (0, -1, 1, 2)[j]
            self.go("L", j, df, 0, 1, True)
            self.go("R", j, df, 0, -1, True)

        def a0(self):
            self.go("l", 0, 0, 0, 1)
            self.go("r", 0, 0, 0, -1)
            self.spread(0)

        def a1l(self):
            self.get("l", 0, -1, 0)
            if self.way > 0:
                self.go("o", 0, -1, 0, 1)
            self.spread(1)

        def a1r(self):
            self.get("r", 0, 1, 0)
            if self.way < 0:
                self.go("o", 0, 1, 0, -1)
            self.spread(2)

        def a2(self):
            self.get("o", 0, 2, 0)
            self.spread(3)

        def b(self, j):
            df = (0, -1, 1, 2)[j]
            if j in (0, 3):
                self.get("L", j, df, -1)
                self.go("O", j, df, -1, 1, True)
            else:
                self.get("R", j, df, 1)
                self.go("O", j, df, 1, -1, True)

        def end(self):
            eight = gl.at[0, 0:2, 0] if self.kind < 2 else w2.at[0, 0, 0:2]
            arrive((self.tag, "end"), eight)

    def unit_of(d):
        return wrap(zh + d, 4)

    def pair(n, d):
        return [Unit(i, unit_of(d), d, *G_WAYS[n][i]) for i in range(2)]

    g = [pair(n, d) for n, d in enumerate((0, 1, 3, 2))]
    v = [
        [
            [Unit(2 + c, u, u, *V_WAYS[c][h][i]) for i, u in enumerate((h, 2 + h))]
            for h in range(2)
        ]
        for c in range(2)
    ]

    def begin():
        gl[zh, y, :, x] = wt[:, rows_for(0), :]
        g[0][0].a0()
        g[0][1].a0()
        exchange_inputs(1)
        exchange_inputs(3)
        for i in range(4):
            tst[i, 0:TB] = tok[i * TB : (i + 1) * TB]
            tst[i, TB : TB + GR] = jnp.broadcast_to(gain[...], (GR, DB))
        for e in (1, 3, 2):
            push(("ta",), "ta", tst.at[wrap(x + e, 4)], tks.at[zl, k, zh, x], device(dx=e))
        tks[zl, k, zh, x] = tst[x]
        for c in range(2):
            w2[c, zh, y, x] = ow[rows_for(0), c * HB : (c + 1) * HB]

    def weights_in(d):
        arrive(("gz", d), gl.at[unit_of(d), y, :, x])

    def outputs_in(c):
        arrive(("wz", c), w2.at[c, 0, 0, 0:3])

    def tokens_first():
        arrive(("ta",), tks.at[0, 0, 0, 0:3])
        own = token_block(0)
        push(("tm", 1), "tm", own, own, device(dz=-1))
        push(("tp", 1), "tp", own, own, device(dz=1))
        push(("s",), "s", own, own, device(dk=1))
        exchange_inputs(2)

    def tokens_down(m):
        block = token_block(m)
        arrive(("tm", m), block)
        if m < 4:
            push(("tm", m + 1), "tm", block, block, device(dz=-1))
        push(("s",), "s", block, block, device(dk=1))

    def tokens_up(m):
        block = token_block(-m)
        arrive(("tp", m), block)
        if m < 3:
            push(("tp", m + 1), "tp", block, block, device(dz=1))
        push(("s",), "s", block, block, device(dk=1))
        if m == 2:
            exchange_outputs()

    def tokens_last():
        arrive(("s",), tks.at[:, 0])

    def normalise():
        spots = [(a, b, c) for a in range(2) for b in range(2) for c in range(4)]

        @pl.loop(0, 4)
        def _(h):
            total = jnp.zeros((TB, DB), F32)
            for a, b, c in spots:
                v = tks[a, b, h, c, 0:TB, :].astype(F32)
                total = total + v * v
            mean = jnp.sum(total, axis=1, keepdims=True) * (1.0 / 4096.0)
            scale = lax.rsqrt(mean + 1e-06)
            rows = pl.ds(pl.multiple_of(h * TB, TB), TB)
            for a, b, c in spots:
                v = tks[a, b, h, c, 0:TB, :].astype(F32)
                g = tks[a, b, h, c, TB : TB + GR, :].astype(F32)[0:1, :]
                nrm[a * 8 + c * 2 + b, rows, :] = (v * scale * g).astype(BF)

    def project(n, t):
        u = g[n][0].u
        for a in range(2):
            right = gl[u, t, a].reshape(4 * FB, DB)
            acc[a] += lax.dot_general(nrm[u * 4 + t], right, NT, preferred_element_type=F32)

    def activate(q):
        @pl.loop(2 * q, 2 * q + 2)
        def _(t):
            rows = pl.ds(pl.multiple_of(t * 64, 64), 64)
            hid[rows, :] = (jax.nn.gelu(acc[0, rows, :], approximate=True) * acc[1, rows, :]).astype(BF)

    def terms(c, h, mine):
        core = k if mine else 1 - k
        for a in range(2):
            blocks = [w2[c, 2 * a + h, 2 * i + core].reshape(4 * FB, HB) for i in range(2)]
            right = jnp.concatenate(blocks, axis=1)
            term = jnp.dot(hid[...], right, preferred_element_type=F32)
            if mine:
                part[c, h, a] = term
            else:
                stx[c, h, a] = term.astype(BF)
                push(("c", c, h), "c", stx.at[c, h, a], srx.at[c, h, a], device(dk=1))

    def ring_value(c, h, i, dz):
        nz = wrap(z + dz, 8)
        a, rows = lax.rem(nz, 2), pl.ds(pl.multiple_of(lax.div(nz, 2) * TB, TB), TB)
        lanes = pl.ds(i * HB, HB)
        return part[c, h, a, rows, lanes] + srx[c, h, a, rows, lanes].astype(F32)

    def own_share(c, h):
        for i in range(2):
            nx = 2 * h + i
            own_tx[c, nx] = ring_value(c, h, i, 0).astype(BF)

            @pl.when(x != nx)
            def _():
                push(("fo", c), "fo", own_tx.at[c, nx], land.at[c, 2, x], owner(0, nx))

            @pl.when(x == nx)
            def _():
                land[c, 2, nx] = own_tx[c, nx]

    def ring_step(c, h, i, s):
        if s == 0 and i == 0:
            arrive(("c", c, h), srx.at[c, h])
        for way in (0, 1):
            length = 4 if h == way else 3
            if s >= length:
                continue
            sign = 1 if way == 0 else -1
            value = ring_value(c, h, i, sign * (length - s))
            if s > 0:
                arrive(("r", c, h, i, way, s - 1), rrx.at[c, h, i, way, s - 1])
                value = value + rrx[c, h, i, way, s - 1].astype(F32)
            rtx[c, h, i, way, s] = value.astype(BF)
            src = rtx.at[c, h, i, way, s]
            if s < length - 1:
                push(("r", c, h, i, way, s), ("r", length), src, rrx.at[c, h, i, way, s], device(dz=sign))
            else:
                push(("fr", c), "fr", src, land.at[c, way, x], owner(sign, 2 * h + i))

    def finish(c):
        arrive(("fr", c), land.at[c, 0:2])
        arrive(("fo", c), land.at[c, 2, 0:3])
        for nx in range(4):
            total = land[c, 0, nx].astype(F32) + land[c, 1, nx].astype(F32)
            total = total + land[c, 2, nx].astype(F32)
            out[nx * TB : (nx + 1) * TB, c * HB : (c + 1) * HB] = total.astype(BF)

    begin()
    g[0][0].a1l()
    g[0][0].a1r()
    g[0][0].b(0)
    g[0][1].b(0)
    g[0][1].a1l()
    g[0][1].a1r()
    g[0][0].b(1)
    g[0][0].a2()
    g[0][0].b(2)
    g[0][1].b(1)
    tokens_first()
    weights_in(3)
    weights_in(1)
    g[1][0].a0()
    g[0][1].b(2)
    g[0][1].a2()
    g[1][1].a0()
    g[0][0].b(3)
    g[1][0].a1r()
    g[1][0].b(0)
    g[1][0].a1l()
    g[1][1].a1l()
    g[1][1].a1r()
    g[0][1].b(3)
    g[0][0].end()
    g[1][0].b(2)
    g[1][1].b(0)
    tokens_down(1)
    tokens_up(1)
    g[1][0].b(1)
    g[2][0].a0()
    g[1][0].a2()
    g[1][1].b(1)
    g[1][1].a2()
    g[1][1].b(2)
    g[2][1].a0()
    g[2][0].a1r()
    g[2][0].b(0)
    g[0][1].end()
    g[1][0].b(3)
    g[2][1].a1l()
    tokens_down(2)
    g[2][0].a1l()
    g[2][1].a1r()
    g[1][1].b(3)
    g[2][0].b(2)
    g[2][1].b(0)
    g[2][0].a2()
    g[1][0].end()
    g[2][0].b(1)
    weights_in(2)
    g[3][0].a0()
    g[2][1].b(1)
    g[2][1].a2()
    g[2][1].b(2)
    g[3][1].a0()
    g[1][1].end()
    g[3][0].a1r()
    g[2][0].b(3)
    tokens_down(3)
    tokens_up(2)
    g[3][0].b(0)
    g[3][0].a1l()
    g[3][1].a1l()
    g[3][1].a1r()
    g[2][1].b(3)
    g[3][0].b(2)
    g[3][1].b(0)
    g[2][0].end()
    g[3][0].b(1)
    g[3][0].a2()
    g[3][1].b(1)
    g[3][1].a2()
    g[3][1].b(2)
    tokens_down(4)
    tokens_up(3)
    g[3][0].b(3)
    g[2][1].end()
    tokens_last()
    outputs_in(0)
    g[3][1].b(3)
    v[0][0][0].a0()
    v[0][0][1].a0()
    normalise()
    v[0][1][0].a0()
    project(0, 0)
    v[0][1][1].a0()
    project(0, 1)
    project(0, 2)
    v[0][0][0].a1r()
    v[0][0][0].b(0)
    project(0, 3)
    v[0][0][1].a1l()
    v[0][0][1].a1r()
    project(1, 0)
    outputs_in(1)
    v[0][0][0].a1l()
    v[0][1][0].a1r()
    v[0][1][0].b(0)
    project(1, 1)
    v[0][0][1].b(0)
    v[0][1][1].a1l()
    v[0][1][1].a1r()
    project(1, 2)
    v[0][0][0].a2()
    v[0][0][0].b(2)
    v[0][1][0].a1l()
    project(1, 3)
    v[0][0][1].b(1)
    v[0][1][1].b(0)
    project(2, 0)
    v[0][0][0].b(1)
    project(2, 1)
    v[0][0][1].b(2)
    v[0][0][1].a2()
    v[0][1][0].b(2)
    project(2, 2)
    v[0][1][0].a2()
    v[0][1][1].a2()
    project(2, 3)
    v[0][1][1].b(1)
    g[3][0].end()
    g[3][1].end()
    v[0][1][1].b(2)
    v[1][0][0].a0()
    project(3, 0)
    v[1][0][1].a0()
    v[0][0][0].b(3)
    project(3, 1)
    v[0][1][0].b(1)
    project(3, 2)
    project(3, 3)
    v[0][0][1].b(3)
    v[0][1][0].b(3)
    activate(0)
    v[1][1][0].a0()
    activate(1)
    v[0][1][1].b(3)
    v[1][0][0].b(0)
    activate(2)
    v[1][0][0].a1l()
    v[1][0][1].a1l()
    activate(3)
    v[1][0][1].b(0)
    v[0][0][0].end()
    v[1][1][1].a0()
    v[1][0][1].a1r()
    v[0][0][1].end()
    v[1][0][0].a1r()
    terms(0, 0, False)
    v[1][1][0].a1l()
    v[1][1][0].b(0)
    terms(0, 0, True)
    v[1][1][0].a1r()
    v[0][1][0].end()
    v[1][0][0].b(1)
    v[0][1][1].end()
    terms(0, 1, False)
    v[1][0][1].b(1)
    terms(0, 1, True)
    v[1][0][1].a2()
    v[1][0][0].b(2)
    ring_step(0, 0, 0, 0)
    ring_step(0, 0, 1, 0)
    v[1][0][1].b(2)
    v[1][1][1].a1r()
    v[1][1][1].a1l()
    v[1][1][0].b(1)
    v[1][1][1].b(0)
    own_share(0, 0)
    v[1][0][0].a2()
    v[1][1][0].b(2)
    v[1][1][0].a2()
    ring_step(0, 1, 0, 0)
    ring_step(0, 1, 1, 0)
    own_share(0, 1)
    v[1][0][1].b(3)
    ring_step(0, 0, 0, 1)
    v[1][1][1].b(2)
    v[1][1][1].a2()
    ring_step(0, 0, 1, 1)
    v[1][1][1].b(1)
    ring_step(0, 1, 0, 1)
    v[1][0][1].end()
    ring_step(0, 1, 1, 1)
    v[1][0][0].b(3)
    v[1][1][0].b(3)
    ring_step(0, 0, 0, 2)
    ring_step(0, 0, 1, 2)
    v[1][1][1].b(3)
    v[1][0][0].end()
    ring_step(0, 1, 0, 2)
    terms(1, 0, False)
    ring_step(0, 1, 1, 2)
    terms(1, 0, True)
    v[1][1][0].end()
    ring_step(0, 0, 0, 3)
    v[1][1][1].end()
    terms(1, 1, False)
    ring_step(0, 0, 1, 3)
    terms(1, 1, True)
    ring_step(1, 0, 0, 0)
    ring_step(1, 0, 1, 0)
    ring_step(0, 1, 0, 3)
    own_share(1, 0)
    ring_step(0, 1, 1, 3)
    ring_step(1, 1, 0, 0)
    ring_step(1, 1, 1, 0)
    own_share(1, 1)
    ring_step(1, 0, 0, 1)
    ring_step(1, 0, 1, 1)
    ring_step(1, 1, 0, 1)
    ring_step(1, 1, 1, 1)
    ring_step(1, 0, 0, 2)
    ring_step(1, 0, 1, 2)
    ring_step(1, 1, 0, 2)
    ring_step(1, 1, 1, 2)
    ring_step(1, 0, 0, 3)
    ring_step(1, 0, 1, 3)
    ring_step(1, 1, 0, 3)
    ring_step(1, 1, 1, 3)
    finish(0)
    finish(1)
    for kind, src in (
        ("ta", tks.at[0, 0, 0, 0:3]),
        ("gz", gl.at[0, 0:3, :, 0]),
        ("wz", w2.at[:, 0, 0, 0:3]),
        (("g", True), gl.at[:, 0:3]),
        (("g", False), gl.at[:, 0:3, :, 0]),
        (("w", True), w2.at[:, :, 0:3]),
        (("w", False), w2.at[:, :, 0:3, 0]),
        ("tm", tks.at[0, 0]),
        ("tp", tks.at[0, 0, 0:3]),
        ("s", tks.at[0]),
        ("c", stx),
        (("r", 4), rtx.at[:, :, :, 0, 0:3]),
        (("r", 3), rtx.at[:, :, :, 0, 0:2]),
        ("fr", rtx.at[:, :, :, :, 0]),
        ("fo", own_tx.at[:, 0:3]),
    ):
        sent(kind, src)
    assert len(ids) == N_RECV and len(kinds) == N_SEND, (len(ids), len(kinds))


def local(tokens, norm_gain, gate_weight, linear_weight, output_weight):
    vmem = pl.BlockSpec(memory_space=pltpu.VMEM)
    return pl.pallas_call(
        kernel,
        out_shape=jax.ShapeDtypeStruct((4 * TB, DB), BF),
        in_specs=[vmem] * 5,
        out_specs=vmem,
        scratch_shapes=[
            pltpu.VMEM((2, 4 * FB, DB), BF),
            pltpu.VMEM((4, 4, 2, 4, FB, DB), BF),
            pltpu.VMEM((2, 4, 4, 4, FB, HB), BF),
            pltpu.VMEM((4, TB + GR, DB), BF),
            pltpu.VMEM((2, 2, 4, 4, TB + GR, DB), BF),
            pltpu.VMEM((16, 4 * TB, DB), BF),
            pltpu.VMEM((2, 4 * TB, 4 * FB), F32),
            pltpu.VMEM((4 * TB, 4 * FB), BF),
            pltpu.VMEM((2, 2, 2, 4 * TB, DB), F32),
            pltpu.VMEM((2, 2, 2, 4 * TB, DB), BF),
            pltpu.VMEM((2, 2, 2, 4 * TB, DB), BF),
            pltpu.VMEM((2, 2, 2, 2, 4, TB, HB), BF),
            pltpu.VMEM((2, 2, 2, 2, 3, TB, HB), BF),
            pltpu.VMEM((2, 4, TB, HB), BF),
            pltpu.VMEM((2, 3, 4, TB, HB), BF),
            pltpu.SemaphoreType.DMA((N_SEND,)),
            pltpu.SemaphoreType.DMA((N_RECV,)),
        ],
        compiler_params=pltpu.CompilerParams(
            collective_id=0, has_side_effects=True, vmem_limit_bytes=60 * 1024 * 1024
        ),
    )(tokens, norm_gain.reshape(1, DB), gate_weight, linear_weight, output_weight)


def solution(mesh):
    return jax.shard_map(
        local,
        mesh=mesh,
        in_specs=(P("row", "col"), P("col"), P("row", "col"), P("row", "col"), P("col", "row")),
        out_specs=P("row", "col"),
        check_vma=False,
    )
```
